512 devices in a mesh: blk: 128 (over z_lo, y, x), freq: 4 (over z_hi, core).
Axes of the slice: x: 4, y: 8, z: 8 (z_hi: 2, z_lo: 4; z = z_hi * 4 + z_lo), core: 2. Of those that a mesh axis runs over, the one named last changes fastest.
Arguments:
- node_index: int32 [3, 16384], P(None, 'blk'), may hold values from 0 to 63
- emitters: int32 [64], replicated, may hold values from 0 to 16383
- admittance: float32 [2, 16384], P(None, 'blk'), may hold values from -3 to 3
- wavenumbers: float32 [4], P('freq'), may hold values from 20 to 60
Outputs:
- scattered: bfloat16 [4, 2, 64, 16384], P('freq', None, None, 'blk')
- gradient: float32 [16384], P('blk')
The draws below stay inside these ranges and needn't reach their ends.
All inputs are finite; a program needn't handle non-finite values.
Results may differ from the reference program's by a relative error of at most 0.006.
Values may be sent and summed in bfloat16 or wider, within the bound.
No kernel may reach another device: no remote copies, remote signals or barrier semaphores. Data moves between devices by JAX's collectives and lax.ppermute only.
A program may use at most 64 MiB of HBM per device.

```python
import math
import jax
import jax.numpy as jnp
from jax import lax

TX = 64
ROWS = 128
GRID = 64
NODES = 16384
FREQS = 4


def plant(entries, rng, smallest, top_value):
    index_at = [jax.random.randint(jax.random.fold_in(rng, axis), (), 0, length) for axis, length in enumerate(entries.shape)]
    longest = entries.shape.index(max(entries.shape))
    beside = index_at[:longest] + [(index_at[longest] + 1) % entries.shape[longest]] + index_at[longest + 1:]
    return entries.at[tuple(index_at)].set(smallest).at[tuple(beside)].set(top_value)


def steps_of(stream_key, dims, shards, least, high):
    def one(dim, shards_of):
        heights = jax.random.uniform(jax.random.fold_in(jax.random.fold_in(stream_key, 6), dim), (shards_of,), jnp.float32, least / len(shards), high / len(shards))
        return jnp.repeat(jnp.exp(heights), dims[dim] // shards_of).reshape((-1,) + (1,) * (len(dims) - dim - 1))

    level = one(*shards[0])
    for cut in shards[1:]:
        level = level * one(*cut)
    return level


def scatter_about(rng, dims, scale, most, split=(), kind=jnp.bfloat16):
    drawn = scale * jax.random.normal(rng, dims, jnp.float32)
    if split:
        drawn = drawn * steps_of(rng, dims, split, -0.22, 0.18)
    return jnp.clip(drawn, -most, most).astype(kind)


def setup_inputs(seed: int = 0) -> dict:
    key_of = jax.random.split(jax.random.key(seed), 5)
    return {
        "node_index": plant(jax.random.randint(key_of[0], (3, NODES), 0, GRID), jax.random.fold_in(key_of[0], 1), 0, GRID - 1).astype(jnp.int32),
        "emitters": plant(jax.random.randint(key_of[1], (TX,), 0, NODES), jax.random.fold_in(key_of[1], 1), 0, NODES - 1).astype(jnp.int32),
        "admittance": scatter_about(key_of[2], (2, NODES), 0.5, 3.0, ((1, 128),), jnp.float32),
        "wavenumbers": jnp.clip(jnp.exp(math.log(60.0) - 1.0986123 * jax.random.uniform(key_of[3], (FREQS,), jnp.float32) ** steps_of(key_of[3], (FREQS,), ((0, 4),), -0.2, 0.2)), 20.0, 60.0),
    }


soften = 0.0025

def green_tile(row_places, col_places, wavenum, strength):
    separation = row_places[:, :, None] - col_places[:, None, :]
    radius = jnp.sqrt(lax.optimization_barrier(jnp.sum(separation * separation, axis=0)) + soften)
    amplitude = strength / radius
    phase_turn = wavenum * radius
    return jnp.stack([amplitude * jnp.cos(phase_turn), amplitude * jnp.sin(phase_turn)]).astype(jnp.bfloat16)

def apply_tile(tile_data, source):
    green_real = tile_data[0].astype(jnp.float32)
    green_imag = tile_data[1].astype(jnp.float32)
    source_real = source[0].astype(jnp.float32)
    source_imag = source[1].astype(jnp.float32)
    high = lax.Precision.HIGHEST
    real_part = jnp.einsum('tc,rc->tr', source_real, green_real, precision=high) - jnp.einsum('tc,rc->tr', source_imag, green_imag, precision=high)
    imag_part = jnp.einsum('tc,rc->tr', source_imag, green_real, precision=high) + jnp.einsum('tc,rc->tr', source_real, green_imag, precision=high)
    return jnp.stack([real_part, imag_part])

def complex_scale(factor_pair, field_pair):
    factor_real = factor_pair[0][None, :]
    factor_imag = factor_pair[1][None, :]
    real_part = factor_real * field_pair[0] - factor_imag * field_pair[1]
    imag_part = factor_real * field_pair[1] + factor_imag * field_pair[0]
    return jnp.stack([real_part, imag_part])

def reference(node_index, emitters, admittance, wavenumbers):
    node_count = node_index.shape[1]
    block_count = node_count // ROWS
    places = node_index.astype(jnp.float32) / GRID
    strength = float(node_count) ** (-0.5)
    emitter_places = places[:, emitters]
    fields = []
    gradient = jnp.zeros((node_count,), jnp.float32)
    for freq_lane in range(FREQS):
        wavenum = wavenumbers[freq_lane]
        incident = green_tile(emitter_places, places, wavenum, 1.0)

        def potential(source):

            def one_block(block_id):
                rows_here = lax.dynamic_slice_in_dim(places, block_id * ROWS, ROWS, 1)
                return apply_tile(green_tile(rows_here, places, wavenum, strength), source)
            stacked = lax.map(one_block, jnp.arange(block_count, dtype=jnp.int32))
            return jnp.transpose(stacked, (1, 2, 0, 3)).reshape(2, TX, node_count)
        first_wave = potential(incident)
        weighted = complex_scale(admittance, first_wave).astype(jnp.bfloat16)
        second = potential(weighted)
        gradient = gradient + lax.optimization_barrier(jnp.sum(first_wave[0] * second[0] - first_wave[1] * second[1], axis=0)) / (FREQS * TX)
        fields.append(second.astype(jnp.bfloat16))
    return (jnp.stack(fields), gradient)
```

```python
import math

import jax
import jax.numpy as jnp
from jax import lax
from jax.experimental import pallas as pl
from jax.experimental.pallas import tpu as pltpu
from jax.sharding import Mesh
from jax.sharding import PartitionSpec as P

GRID = 64
BLK = ("z", "y", "x")
GATHER = ("z", "x")
REDUCE = "y"
LANES = 128
FEATURES = 16
SOFT = 0.0025 * GRID * GRID
MAGIC = 12582912.0
ROOT2 = math.sqrt(2.0)
SIN_POLY = [ROOT2 * c for c in (3.1415820221197075, -5.167142794757069, 2.541899010399708, -0.554636148527055)]
COS_POLY = [ROOT2 * c for c in (0.9999933001981278, -4.933938170377516, 4.04128504935244, -1.2221298133692595)]


def poly(coefs, s):
    total = coefs[-1] * s + coefs[-2]
    for c in coefs[-3::-1]:
        total = total * s + c
    return total


def green_parts(square, turns_per_step):
    v = square + SOFT
    inv = lax.rsqrt(v)
    turns = (v * inv) * turns_per_step
    f = turns - ((turns + MAGIC) - MAGIC)
    s = f * f
    half_sin = poly(SIN_POLY, s) * f
    half_cos = poly(COS_POLY, s)
    q = inv * half_sin
    return inv - q * half_sin, q * half_cos


def centred(places):
    return places.astype(jnp.float32) - 32.0


def column_features(places):
    p = centred(places)
    n = jnp.sum(p * p, axis=0, keepdims=True)
    high = ((n * (1 / 64) + MAGIC) - MAGIC) * 64.0
    low = n - high
    one = jnp.ones_like(n)
    zero = jnp.zeros((FEATURES - 7, n.shape[1]), jnp.float32)
    return jnp.concatenate([p * -2.0, one, one, high, low, zero], axis=0)


def row_features(x, y, z):
    lane = lax.broadcasted_iota(jnp.int32, x.shape, 1)
    x, y, z = x - 32.0, y - 32.0, z - 32.0
    n = x * x + y * y + z * z
    high = ((n * (1 / 64) + MAGIC) - MAGIC) * 64.0
    low = n - high
    out = jnp.where(lane == 0, x, 0.0)
    out = jnp.where(lane == 1, y, out)
    out = jnp.where(lane == 2, z, out)
    out = jnp.where(lane == 3, high, out)
    out = jnp.where(lane == 4, low, out)
    return jnp.where((lane == 5) | (lane == 6), 1.0, out)


def dot(a, b, contract=((1,), (0,))):
    return lax.dot_general(a, b, (contract, ((), ())), preferred_element_type=jnp.float32)


NT = ((1,), (1,))


def rows_of(places):
    count = places.shape[1]
    spread = []
    for d in range(3):
        line = jnp.broadcast_to(places[d : d + 1, :].astype(jnp.float32), (LANES, count))
        spread.append(jnp.transpose(line))
    return spread


def first_kernel(turns_ref, places_ref, own_ref, emitters_ref, admittance_ref, first_ref, weighted_ref,
                 cols_ref, rows_ref, d0, d1, g0, g1, acc_ref):
    blocks = places_ref.shape[0]
    own = own_ref.shape[1]
    emitters = emitters_ref.shape[0]
    width = d0.shape[1]
    per = width // own
    chunks = blocks // per
    turns = turns_ref[0] * (1.0 / (GRID * 2.0 * math.pi))

    rows_ref[0:own] = row_features(*rows_of(own_ref[...])).astype(jnp.bfloat16)
    index = jnp.broadcast_to(emitters_ref[...], (emitters, LANES))
    lane = lax.broadcasted_iota(jnp.int32, (emitters, LANES), 1)
    of_block = jnp.where(lane == index // own, 1.0, 0.0).astype(jnp.bfloat16)
    at_lane = lane == index % own
    every = jnp.ones((LANES, LANES), jnp.bfloat16)
    found = []
    for d in range(3):
        line = dot(of_block, places_ref[:, d, :])
        found.append(dot(jnp.where(at_lane, line, 0.0).astype(jnp.bfloat16), every))
    rows_ref[own : own + emitters] = row_features(*found).astype(jnp.bfloat16)

    acc_ref[...] = jnp.zeros_like(acc_ref)

    def distances(chunk, d_ref):
        for b in range(per):
            cols = column_features(places_ref[chunk * per + b]).astype(jnp.bfloat16)
            d_ref[:, b * own : (b + 1) * own] = dot(rows_ref[:, 0:FEATURES], cols)

    def tile(d_ref, g_ref):
        for r in range(0, own + emitters, 16):
            real, imag = green_parts(d_ref[r : r + 16, :], turns)
            at = r if r < own else r + own
            step = own if r < own else emitters
            g_ref[at : at + 16, :] = real.astype(jnp.bfloat16)
            g_ref[at + step : at + step + 16, :] = imag.astype(jnp.bfloat16)

    def gather(g_ref):
        acc_ref[...] += dot(g_ref[2 * own :, :], g_ref[0 : 2 * own, :], NT)

    distances(0, d0)
    g1[...] = jnp.zeros_like(g1)

    def pair(i, carry):
        distances(2 * i + 1, d1)
        tile(d0, g0)
        gather(g1)
        distances(jnp.minimum(2 * i + 2, chunks - 1), d0)
        tile(d1, g1)
        gather(g0)
        return carry

    lax.fori_loop(0, chunks // 2, pair, 0)
    gather(g1)
    scale = (GRID * GRID) * float(blocks * own) ** (-0.5)
    top, low = acc_ref[0:emitters, :], acc_ref[emitters:, :]
    real = (top[:, 0:own] - low[:, own:]) * scale
    imag = (low[:, 0:own] + top[:, own:]) * scale
    first_ref[0] = real
    first_ref[1] = imag
    a, b = admittance_ref[0:1, :], admittance_ref[1:2, :]
    w_real = (a * real - b * imag).astype(jnp.bfloat16)
    w_imag = (a * imag + b * real).astype(jnp.bfloat16)
    for k in range(weighted_ref.shape[0]):
        weighted_ref[k, 0] = w_real
        weighted_ref[k, 1] = w_imag


def second_kernel(turns_ref, row_places_ref, col_places_ref, source_ref, part_ref,
                  cols_ref, rows_ref, d0, d1, r0, i0, r1, i1, acc_r, acc_i, *, node_count):
    groups, _, own = col_places_ref.shape
    targets = row_places_ref.shape[0]
    emitters = source_ref.shape[2]
    width = targets * own
    turns = turns_ref[0] * (1.0 / (GRID * 2.0 * math.pi))
    for b in range(targets):
        cols_ref[:, b * own : (b + 1) * own] = column_features(row_places_ref[b]).astype(jnp.bfloat16)
    acc_r[...] = jnp.zeros_like(acc_r)
    acc_i[...] = jnp.zeros_like(acc_i)

    def distances(c, d_ref):
        rows = row_features(*rows_of(col_places_ref[c])).astype(jnp.bfloat16)
        d_ref[...] = dot(rows[:, 0:FEATURES], cols_ref[...])

    def tile(d_ref, r_ref, i_ref):
        for r in range(0, own, 16):
            for w in range(0, width, 512):
                real, imag = green_parts(d_ref[r : r + 16, w : w + 512], turns)
                r_ref[r : r + 16, w : w + 512] = real.astype(jnp.bfloat16)
                i_ref[r : r + 16, w : w + 512] = imag.astype(jnp.bfloat16)

    def gather(c, r_ref, i_ref):
        lhs = source_ref[c].reshape(2 * emitters, own)
        acc_r[...] += dot(lhs, r_ref[...])
        acc_i[...] += dot(lhs, i_ref[...])

    distances(0, d0)
    r1[...] = jnp.zeros_like(r1)
    i1[...] = jnp.zeros_like(i1)

    def pair(k, carry):
        distances(2 * k + 1, d1)
        tile(d0, r0, i0)
        gather(jnp.maximum(2 * k - 1, 0), r1, i1)
        distances(jnp.minimum(2 * k + 2, groups - 1), d0)
        tile(d1, r1, i1)
        gather(2 * k, r0, i0)
        return carry

    lax.fori_loop(0, groups // 2, pair, 0)
    gather(groups - 1, r1, i1)
    scale = GRID * float(node_count) ** (-0.5)
    for b in range(targets):
        at = slice(b * own, (b + 1) * own)
        part_ref[b, 0] = ((acc_r[0:emitters, at] - acc_i[emitters:, at]) * scale).astype(part_ref.dtype)
        part_ref[b, 1] = ((acc_r[emitters:, at] + acc_i[0:emitters, at]) * scale).astype(part_ref.dtype)


def last_kernel(parts_ref, first_ref, second_ref, terms_ref, *, share):
    real = parts_ref[0, 0].astype(jnp.float32)
    imag = parts_ref[0, 1].astype(jnp.float32)
    for b in range(1, parts_ref.shape[0]):
        real += parts_ref[b, 0].astype(jnp.float32)
        imag += parts_ref[b, 1].astype(jnp.float32)
    second_ref[0, 0] = real.astype(jnp.bfloat16)
    second_ref[0, 1] = imag.astype(jnp.bfloat16)
    terms = jnp.sum(first_ref[0] * real - first_ref[1] * imag, axis=0, keepdims=True) * share
    terms_ref[...] = jnp.broadcast_to(terms[None], terms_ref.shape)


VMEM = pl.BlockSpec(memory_space=pltpu.VMEM)
SMEM = pl.BlockSpec(memory_space=pltpu.SMEM)


def local(node_index, emitters, admittance, wavenumbers):
    sizes = [lax.axis_size(a) for a in BLK]
    blocks = sizes[0] * sizes[1] * sizes[2]
    lanes = lax.axis_size("freq")
    own = node_index.shape[1]
    count = blocks * own
    tx = emitters.shape[0]
    near, far = lax.axis_size(GATHER), lax.axis_size(REDUCE)

    own_places = node_index.astype(jnp.bfloat16)
    copies = jnp.broadcast_to(own_places, (blocks, *own_places.shape))
    places = lax.all_to_all(copies, BLK, split_axis=0, concat_axis=0, tiled=True)
    f32, bf16 = jnp.float32, jnp.bfloat16
    width = 4 * own
    first, weighted = pl.pallas_call(
        first_kernel,
        out_shape=(
            jax.ShapeDtypeStruct((2, tx, own), f32),
            jax.ShapeDtypeStruct((near, 2, tx, own), bf16),
        ),
        in_specs=[SMEM, VMEM, VMEM, VMEM, VMEM],
        out_specs=(VMEM, VMEM),
        scratch_shapes=[
            pltpu.VMEM((FEATURES, width), bf16),
            pltpu.VMEM((own + tx, LANES), bf16),
            pltpu.VMEM((own + tx, width), f32),
            pltpu.VMEM((own + tx, width), f32),
            pltpu.VMEM((2 * (own + tx), width), bf16),
            pltpu.VMEM((2 * (own + tx), width), bf16),
            pltpu.VMEM((2 * tx, 2 * own), f32),
        ],
        name="first_wave",
    )(wavenumbers, places, own_places, emitters[:, None], admittance)

    grouped = places.reshape(*sizes, 3, own)
    row_places = lax.dynamic_index_in_dim(
        lax.dynamic_index_in_dim(grouped, lax.axis_index("z"), 0, False), lax.axis_index("x"), 1, False
    )
    col_places = lax.dynamic_index_in_dim(grouped, lax.axis_index("y"), 1, False).reshape(near, 3, own)
    source = lax.all_to_all(weighted, GATHER, split_axis=0, concat_axis=0, tiled=True)
    import functools

    part = pl.pallas_call(
        functools.partial(second_kernel, node_count=count),
        out_shape=jax.ShapeDtypeStruct((far, 2, tx, own), bf16),
        in_specs=[SMEM, VMEM, VMEM, VMEM],
        out_specs=VMEM,
        scratch_shapes=[
            pltpu.VMEM((FEATURES, far * own), bf16),
            pltpu.VMEM((own, LANES), bf16),
            pltpu.VMEM((own, far * own), f32),
            pltpu.VMEM((own, far * own), f32),
            pltpu.VMEM((own, far * own), bf16),
            pltpu.VMEM((own, far * own), bf16),
            pltpu.VMEM((own, far * own), bf16),
            pltpu.VMEM((own, far * own), bf16),
            pltpu.VMEM((2 * tx, far * own), f32),
            pltpu.VMEM((2 * tx, far * own), f32),
        ],
        name="second_wave",
    )(wavenumbers, row_places, col_places, source)
    parts = lax.all_to_all(part, REDUCE, split_axis=0, concat_axis=0, tiled=True)
    second, terms = pl.pallas_call(
        functools.partial(last_kernel, share=1.0 / (lanes * tx)),
        out_shape=(
            jax.ShapeDtypeStruct((1, 2, tx, own), bf16),
            jax.ShapeDtypeStruct((lanes, 1, own), f32),
        ),
        in_specs=[VMEM, VMEM],
        out_specs=(VMEM, VMEM),
        name="last_sum",
    )(parts, first)
    terms = lax.all_to_all(terms, "freq", split_axis=0, concat_axis=0, tiled=True)
    return second, terms.sum(axis=(0, 1))


def solution(mesh):
    split = Mesh(mesh.devices.reshape(4, 8, 4, mesh.shape["freq"]), ("z", "y", "x", "freq"))
    in_specs = (P(None, BLK), P(), P(None, BLK), P("freq"))
    out_specs = (P("freq", None, None, BLK), P(BLK))
    return jax.shard_map(local, mesh=split, in_specs=in_specs, out_specs=out_specs, check_vma=False)
```

```python
import functools
import math

import jax
import jax.numpy as jnp
from jax import lax
from jax.experimental import pallas as pl
from jax.experimental.pallas import tpu as pltpu
from jax.sharding import Mesh
from jax.sharding import PartitionSpec as P

GRID = 64
BLK = ("z", "y", "x")
GATHER = ("z", "x")
REDUCE = "y"
LANES = 128
FEATURES = 16
SOFT = 0.0025 * GRID * GRID
MAGIC = 12582912.0
ROOT2 = math.sqrt(2.0)
SIN_POLY = [ROOT2 * c for c in (3.1415820221197075, -5.167142794757069, 2.541899010399708, -0.554636148527055)]
COS_POLY = [ROOT2 * c for c in (0.9999933001981278, -4.933938170377516, 4.04128504935244, -1.2221298133692595)]


def poly(coefs, s):
    total = coefs[-1] * s + coefs[-2]
    for c in coefs[-3::-1]:
        total = total * s + c
    return total


def green_parts(square, turns_per_step):
    v = square + SOFT
    inv = lax.rsqrt(v)
    turns = (v * inv) * turns_per_step
    f = turns - ((turns + MAGIC) - MAGIC)
    s = f * f
    half_sin = poly(SIN_POLY, s) * f
    half_cos = poly(COS_POLY, s)
    q = inv * half_sin
    return inv - q * half_sin, q * half_cos


def centred(places):
    return places.astype(jnp.float32) - 32.0


def column_features(places):
    p = centred(places)
    n = jnp.sum(p * p, axis=0, keepdims=True)
    high = ((n * (1 / 64) + MAGIC) - MAGIC) * 64.0
    low = n - high
    one = jnp.ones_like(n)
    zero = jnp.zeros((FEATURES - 7, n.shape[1]), jnp.float32)
    return jnp.concatenate([p * -2.0, one, one, high, low, zero], axis=0)


def row_features(x, y, z):
    lane = lax.broadcasted_iota(jnp.int32, x.shape, 1)
    x, y, z = x - 32.0, y - 32.0, z - 32.0
    n = x * x + y * y + z * z
    high = ((n * (1 / 64) + MAGIC) - MAGIC) * 64.0
    low = n - high
    out = jnp.where(lane == 0, x, 0.0)
    out = jnp.where(lane == 1, y, out)
    out = jnp.where(lane == 2, z, out)
    out = jnp.where(lane == 3, high, out)
    out = jnp.where(lane == 4, low, out)
    return jnp.where((lane == 5) | (lane == 6), 1.0, out)


def dot(a, b, contract=((1,), (0,))):
    return lax.dot_general(a, b, (contract, ((), ())), preferred_element_type=jnp.float32)


NT = ((1,), (1,))


def rows_of(places):
    count = places.shape[1]
    spread = []
    for d in range(3):
        line = jnp.broadcast_to(places[d : d + 1, :].astype(jnp.float32), (LANES, count))
        spread.append(jnp.transpose(line))
    return spread


def start_kernel(wavenumber_ref, own_ref, emitters_ref, admittance_ref, copies_ref, rows_ref, index_ref, side_ref):
    own = own_ref[...].astype(jnp.bfloat16)
    copies_ref[...] = jnp.broadcast_to(own[None], copies_ref.shape)
    rows_ref[...] = row_features(*rows_of(own)).astype(jnp.bfloat16)
    emitters = jnp.broadcast_to(emitters_ref[...].astype(jnp.float32), (LANES, emitters_ref.shape[1]))
    index_ref[...] = jnp.transpose(emitters).astype(jnp.int32)
    turns = wavenumber_ref[...] * (1.0 / (GRID * 2.0 * math.pi))
    side_ref[...] = jnp.broadcast_to(turns, side_ref.shape)
    side_ref[1:3] = admittance_ref[...]


def first_kernel(side_ref, places_ref, own_rows_ref, index_ref, first_ref, weighted_ref,
                 rows_ref, d0, d1, g0, g1, acc_ref):
    blocks = places_ref.shape[0]
    own = own_rows_ref.shape[0]
    emitters = index_ref.shape[0]
    width = d0.shape[1]
    per = width // own
    chunks = blocks // per
    turns = side_ref[0:1, 0:1]

    rows_ref[0:own] = own_rows_ref[...]
    index = index_ref[...]
    lane = lax.broadcasted_iota(jnp.int32, (emitters, LANES), 1)
    of_block = jnp.where(lane == index // own, 1.0, 0.0).astype(jnp.bfloat16)
    at_lane = lane == index % own
    every = jnp.ones((LANES, LANES), jnp.bfloat16)
    found = []
    for d in range(3):
        line = dot(of_block, places_ref[:, d, :])
        found.append(dot(jnp.where(at_lane, line, 0.0).astype(jnp.bfloat16), every))
    rows_ref[own : own + emitters] = row_features(*found).astype(jnp.bfloat16)

    acc_ref[...] = jnp.zeros_like(acc_ref)

    def distances(chunk, d_ref):
        for b in range(per):
            cols = column_features(places_ref[chunk * per + b]).astype(jnp.bfloat16)
            d_ref[:, b * own : (b + 1) * own] = dot(rows_ref[:, 0:FEATURES], cols)

    def tile(d_ref, g_ref):
        for r in range(0, own + emitters, 16):
            real, imag = green_parts(d_ref[r : r + 16, :], turns)
            at = r if r < own else r + own
            step = own if r < own else emitters
            g_ref[at : at + 16, :] = real.astype(jnp.bfloat16)
            g_ref[at + step : at + step + 16, :] = imag.astype(jnp.bfloat16)

    def gather(g_ref):
        acc_ref[...] += dot(g_ref[2 * own :, :], g_ref[0 : 2 * own, :], NT)

    distances(0, d0)
    g1[...] = jnp.zeros_like(g1)

    def pair(i, carry):
        distances(2 * i + 1, d1)
        tile(d0, g0)
        gather(g1)
        distances(jnp.minimum(2 * i + 2, chunks - 1), d0)
        tile(d1, g1)
        gather(g0)
        return carry

    lax.fori_loop(0, chunks // 2, pair, 0)
    gather(g1)
    scale = (GRID * GRID) * float(blocks * own) ** (-0.5)
    top, low = acc_ref[0:emitters, :], acc_ref[emitters:, :]
    real = (top[:, 0:own] - low[:, own:]) * scale
    imag = (low[:, 0:own] + top[:, own:]) * scale
    first_ref[0] = real
    first_ref[1] = imag
    a, b = side_ref[1:2, :], side_ref[2:3, :]
    w_real = (a * real - b * imag).astype(jnp.bfloat16)
    w_imag = (a * imag + b * real).astype(jnp.bfloat16)
    for k in range(weighted_ref.shape[0]):
        weighted_ref[k, 0] = w_real
        weighted_ref[k, 1] = w_imag


def tile_kernel(side_ref, places_ref, after_ref, tile_ref, cols_ref, d0, d1, t0, t1, sems, *, sizes):
    nz, ny, nx = sizes
    own = places_ref.shape[2]
    width = ny * own
    iz, iy, ix = (lax.axis_index(a) for a in BLK)
    turns = side_ref[0:1, 0:1]
    for b in range(ny):
        block = (iz * ny + b) * nx + ix
        cols_ref[:, b * own : (b + 1) * own] = column_features(places_ref[block]).astype(jnp.bfloat16)

    def distances(c, d_ref):
        block = ((c // nx) * ny + iy) * nx + c % nx
        rows = row_features(*rows_of(places_ref[block])).astype(jnp.bfloat16)
        d_ref[...] = dot(rows[:, 0:FEATURES], cols_ref[...])

    def tile(d_ref, t_ref):
        for r in range(0, own, 16):
            for w in range(0, width, 512):
                real, imag = green_parts(d_ref[r : r + 16, w : w + 512], turns)
                t_ref[0, r : r + 16, w : w + 512] = real.astype(jnp.bfloat16)
                t_ref[1, r : r + 16, w : w + 512] = imag.astype(jnp.bfloat16)

    def out(c, t_ref, s):
        return pltpu.make_async_copy(t_ref, tile_ref.at[c], sems.at[s])

    distances(0, d0)

    def pair(k, carry):
        @pl.when(k > 0)
        def _():
            out(2 * k - 2, t0, 0).wait()

        distances(2 * k + 1, d1)
        tile(d0, t0)
        out(2 * k, t0, 0).start()

        @pl.when(k > 0)
        def _():
            out(2 * k - 1, t1, 1).wait()

        distances(jnp.minimum(2 * k + 2, nz * nx - 1), d0)
        tile(d1, t1)
        out(2 * k + 1, t1, 1).start()
        return carry

    lax.fori_loop(0, nz * nx // 2, pair, 0)
    out(nz * nx - 2, t0, 0).wait()
    out(nz * nx - 1, t1, 1).wait()


def second_kernel(source_ref, tile_ref, part_ref, lhs_ref, all_ref, acc_r, acc_i, sems, *, node_count):
    groups, _, emitters, own = source_ref.shape
    targets = part_ref.shape[0]
    pieces = sems.shape[0]
    per = groups // pieces

    def bring(p):
        at = pl.ds(p * per, per)
        return pltpu.make_async_copy(tile_ref.at[at], all_ref.at[at], sems.at[p])

    for p in range(pieces):
        bring(p).start()
    for c in range(groups):
        lhs_ref[:, c * own : (c + 1) * own] = source_ref[c].reshape(2 * emitters, own)
    for p in range(pieces):
        bring(p).wait()
        lhs = lhs_ref[:, p * per * own : (p + 1) * per * own]
        for part, acc in ((0, acc_r), (1, acc_i)):
            rhs = all_ref[p * per : (p + 1) * per, part].reshape(per * own, targets * own)
            here = dot(lhs, rhs)
            acc[...] = here if p == 0 else acc[...] + here
    scale = GRID * float(node_count) ** (-0.5)
    for b in range(targets):
        at = slice(b * own, (b + 1) * own)
        part_ref[b, 0] = ((acc_r[0:emitters, at] - acc_i[emitters:, at]) * scale).astype(part_ref.dtype)
        part_ref[b, 1] = ((acc_r[emitters:, at] + acc_i[0:emitters, at]) * scale).astype(part_ref.dtype)


def last_kernel(parts_ref, first_ref, second_ref, terms_ref, *, share):
    real = parts_ref[0, 0].astype(jnp.float32)
    imag = parts_ref[0, 1].astype(jnp.float32)
    for b in range(1, parts_ref.shape[0]):
        real += parts_ref[b, 0].astype(jnp.float32)
        imag += parts_ref[b, 1].astype(jnp.float32)
    second_ref[0, 0] = real.astype(jnp.bfloat16)
    second_ref[0, 1] = imag.astype(jnp.bfloat16)
    terms = jnp.sum(first_ref[0] * real - first_ref[1] * imag, axis=0, keepdims=True) * share
    terms_ref[...] = jnp.broadcast_to(terms[None], terms_ref.shape)


VMEM = pl.BlockSpec(memory_space=pltpu.VMEM)
HBM = pl.BlockSpec(memory_space=pltpu.HBM)


def limit(mib):
    return pltpu.CompilerParams(vmem_limit_bytes=mib << 20)


def local(node_index, emitters, admittance, wavenumbers):
    sizes = [lax.axis_size(a) for a in BLK]
    blocks = sizes[0] * sizes[1] * sizes[2]
    lanes = lax.axis_size("freq")
    own = node_index.shape[1]
    count = blocks * own
    tx = emitters.shape[0]
    near, far = lax.axis_size(GATHER), lax.axis_size(REDUCE)

    f32, bf16 = jnp.float32, jnp.bfloat16
    copies, own_rows, index, side = pl.pallas_call(
        start_kernel,
        out_shape=(
            jax.ShapeDtypeStruct((blocks, 3, own), bf16),
            jax.ShapeDtypeStruct((own, LANES), bf16),
            jax.ShapeDtypeStruct((tx, LANES), jnp.int32),
            jax.ShapeDtypeStruct((8, own), f32),
        ),
        in_specs=[VMEM] * 4,
        out_specs=(VMEM,) * 4,
        compiler_params=limit(4),
        name="start",
    )(wavenumbers[None], node_index, emitters[None], admittance)
    places = lax.all_to_all(copies, BLK, split_axis=0, concat_axis=0, tiled=True)
    width = 4 * own
    first, weighted = pl.pallas_call(
        first_kernel,
        out_shape=(
            jax.ShapeDtypeStruct((2, tx, own), f32),
            jax.ShapeDtypeStruct((near, 2, tx, own), bf16),
        ),
        in_specs=[VMEM] * 4,
        out_specs=(VMEM, VMEM),
        scratch_shapes=[
            pltpu.VMEM((own + tx, LANES), bf16),
            pltpu.VMEM((own + tx, width), f32),
            pltpu.VMEM((own + tx, width), f32),
            pltpu.VMEM((2 * (own + tx), width), bf16),
            pltpu.VMEM((2 * (own + tx), width), bf16),
            pltpu.VMEM((2 * tx, 2 * own), f32),
        ],
        compiler_params=limit(8),
        name="first_wave",
    )(side, places, own_rows, index)

    source = lax.all_to_all(weighted, GATHER, split_axis=0, concat_axis=0, tiled=True)
    tile = pl.pallas_call(
        functools.partial(tile_kernel, sizes=sizes),
        out_shape=jax.ShapeDtypeStruct((near, 2, own, far * own), bf16),
        in_specs=[VMEM, VMEM, pl.BlockSpec(memory_space=pl.ANY)],
        out_specs=HBM,
        scratch_shapes=[
            pltpu.VMEM((FEATURES, far * own), bf16),
            pltpu.VMEM((own, far * own), f32),
            pltpu.VMEM((own, far * own), f32),
            pltpu.VMEM((2, own, far * own), bf16),
            pltpu.VMEM((2, own, far * own), bf16),
            pltpu.SemaphoreType.DMA((2,)),
        ],
        compiler_params=limit(50),
        cost_estimate=pl.CostEstimate(flops=10**10, bytes_accessed=1 << 23, transcendentals=1 << 21),
        name="green_tile",
    )(side, places, first)
    part = pl.pallas_call(
        functools.partial(second_kernel, node_count=count),
        out_shape=jax.ShapeDtypeStruct((far, 2, tx, own), bf16),
        in_specs=[VMEM, HBM],
        out_specs=VMEM,
        scratch_shapes=[
            pltpu.VMEM((2 * tx, near * own), bf16),
            pltpu.VMEM((near, 2, own, far * own), bf16),
            pltpu.VMEM((2 * tx, far * own), f32),
            pltpu.VMEM((2 * tx, far * own), f32),
            pltpu.SemaphoreType.DMA((4,)),
        ],
        compiler_params=limit(50),
        name="second_wave",
    )(source, tile)
    parts = lax.all_to_all(part, REDUCE, split_axis=0, concat_axis=0, tiled=True)
    second, terms = pl.pallas_call(
        functools.partial(last_kernel, share=1.0 / (lanes * tx)),
        out_shape=(
            jax.ShapeDtypeStruct((1, 2, tx, own), bf16),
            jax.ShapeDtypeStruct((lanes, 1, own), f32),
        ),
        in_specs=[VMEM, VMEM],
        out_specs=(VMEM, VMEM),
        compiler_params=limit(4),
        name="last_sum",
    )(parts, first)
    terms = lax.all_to_all(terms, "freq", split_axis=0, concat_axis=0, tiled=True)
    return second, terms.sum(axis=(0, 1))


def solution(mesh):
    split = Mesh(mesh.devices.reshape(4, 8, 4, mesh.shape["freq"]), ("z", "y", "x", "freq"))
    in_specs = (P(None, BLK), P(), P(None, BLK), P("freq"))
    out_specs = (P("freq", None, None, BLK), P(BLK))
    return jax.shard_map(local, mesh=split, in_specs=in_specs, out_specs=out_specs, check_vma=False)
```

```python
import functools
import math

import jax
import jax.numpy as jnp
from jax import lax
from jax.experimental import pallas as pl
from jax.experimental.pallas import tpu as pltpu
from jax.sharding import Mesh
from jax.sharding import PartitionSpec as P

GRID = 64
BLK = ("zs", "za", "y", "x")
GATHER = ("zs", "y")
REDUCE = ("za", "x")
LANES = 128
FEATURES = 16
SOFT = 0.0025 * GRID * GRID
MAGIC = 12582912.0
ROOT2 = math.sqrt(2.0)
SIN_POLY = [ROOT2 * c for c in (3.1415820221197075, -5.167142794757069, 2.541899010399708, -0.554636148527055)]
COS_POLY = [ROOT2 * c for c in (0.9999933001981278, -4.933938170377516, 4.04128504935244, -1.2221298133692595)]


def poly(coefs, s):
    total = coefs[-1] * s + coefs[-2]
    for c in coefs[-3::-1]:
        total = total * s + c
    return total


def green_parts(square, turns_per_step):
    v = square + SOFT
    inv = lax.rsqrt(v)
    turns = (v * inv) * turns_per_step
    f = turns - ((turns + MAGIC) - MAGIC)
    s = f * f
    half_sin = poly(SIN_POLY, s) * f
    half_cos = poly(COS_POLY, s)
    q = inv * half_sin
    return inv - q * half_sin, q * half_cos


def split_norm(p):
    n = jnp.sum(p * p, axis=0, keepdims=True)
    high = ((n * (1 / 64) + MAGIC) - MAGIC) * 64.0
    return high, n - high


def features(places, target):
    p = places.astype(jnp.float32) - 32.0
    high, low = split_norm(p)
    one = jnp.ones_like(high)
    zero = jnp.zeros((FEATURES - 7, p.shape[1]), jnp.float32)
    if target:
        return jnp.concatenate([p, high, low, one, one, zero], axis=0)
    return jnp.concatenate([p * -2.0, one, one, high, low, zero], axis=0)


def spread_features(x, y, z):
    lane = lax.broadcasted_iota(jnp.int32, x.shape, 1)
    x, y, z = x - 32.0, y - 32.0, z - 32.0
    n = x * x + y * y + z * z
    high = ((n * (1 / 64) + MAGIC) - MAGIC) * 64.0
    low = n - high
    out = jnp.where(lane == 0, x, 0.0)
    out = jnp.where(lane == 1, y, out)
    out = jnp.where(lane == 2, z, out)
    out = jnp.where(lane == 3, high, out)
    out = jnp.where(lane == 4, low, out)
    return jnp.where((lane == 5) | (lane == 6), 1.0, out)


def dot(a, b, contract=((1,), (0,))):
    return lax.dot_general(a, b, (contract, ((), ())), preferred_element_type=jnp.float32)


def start_kernel(wavenumber_ref, node_ref, emitters_ref, admittance_ref, own_ref, index_ref, side_ref):
    own_ref[...] = features(node_ref[...], True).astype(jnp.bfloat16)
    emitters = jnp.broadcast_to(emitters_ref[...].astype(jnp.float32), (LANES, emitters_ref.shape[1]))
    index_ref[...] = jnp.transpose(emitters).astype(jnp.int32)
    side_ref[0:2] = admittance_ref[...]
    turns = wavenumber_ref[0] * (1.0 / (GRID * 2.0 * math.pi))
    side_ref[2:8] = jnp.full((6, side_ref.shape[1]), turns, jnp.float32)


def first_kernel(side_ref, places_ref, own_ref, index_ref, first_ref, weighted_ref,
                 rows_ref, d0, d1, g0, g1, acc_ref):
    blocks = places_ref.shape[0]
    own = own_ref.shape[1]
    emitters = index_ref.shape[0]
    width = d0.shape[1]
    per = width // own
    chunks = blocks // per
    turns = side_ref[6:7, 0:1]

    rows_ref[0:own, 0:FEATURES] = jnp.transpose(own_ref[...].astype(jnp.float32)).astype(jnp.bfloat16)
    index = index_ref[...]
    lane = lax.broadcasted_iota(jnp.int32, (emitters, LANES), 1)
    of_block = jnp.where(lane == index // own, 1.0, 0.0).astype(jnp.bfloat16)
    at_lane = lane == index % own
    every = jnp.ones((LANES, LANES), jnp.bfloat16)
    found = []
    for d in range(3):
        line = dot(of_block, places_ref[:, d, :])
        found.append(dot(jnp.where(at_lane, line, 0.0).astype(jnp.bfloat16), every))
    rows_ref[own : own + emitters] = spread_features(*found).astype(jnp.bfloat16)

    acc_ref[...] = jnp.zeros_like(acc_ref)

    def distances(chunk, d_ref):
        for b in range(per):
            psi = features(places_ref[chunk * per + b], False).astype(jnp.bfloat16)
            d_ref[:, b * own : (b + 1) * own] = dot(rows_ref[:, 0:FEATURES], psi)

    def tile(d_ref, g_ref):
        for r in range(0, own + emitters, 16):
            at = r if r < own else r + own
            step = own if r < own else emitters
            for w in range(0, width, 512):
                real, imag = green_parts(d_ref[r : r + 16, w : w + 512], turns)
                g_ref[at : at + 16, w : w + 512] = real.astype(jnp.bfloat16)
                g_ref[at + step : at + step + 16, w : w + 512] = imag.astype(jnp.bfloat16)

    def gather(g_ref):
        acc_ref[...] += dot(g_ref[2 * own :, :], g_ref[0 : 2 * own, :], ((1,), (1,)))

    distances(0, d0)
    g1[...] = jnp.zeros_like(g1)

    def pair(i, carry):
        distances(2 * i + 1, d1)
        tile(d0, g0)
        gather(g1)
        distances(jnp.minimum(2 * i + 2, chunks - 1), d0)
        tile(d1, g1)
        gather(g0)
        return carry

    lax.fori_loop(0, chunks // 2, pair, 0)
    gather(g1)
    scale = (GRID * GRID) * float(blocks * own) ** (-0.5)
    top, low = acc_ref[0:emitters, :], acc_ref[emitters:, :]
    real = (top[:, 0:own] - low[:, own:]) * scale
    imag = (low[:, 0:own] + top[:, own:]) * scale
    first_ref[0] = real
    first_ref[1] = imag
    a, b = side_ref[0:1, :], side_ref[1:2, :]
    w_real = (a * real - b * imag).astype(jnp.bfloat16)
    w_imag = (a * imag + b * real).astype(jnp.bfloat16)
    for k in range(weighted_ref.shape[0]):
        weighted_ref[k, 0] = w_real
        weighted_ref[k, 1] = w_imag


def block_at(where, sizes):
    place = 0
    for a in BLK:
        place = place * sizes[a] + where[a]
    return place


def unravel(k, axes, sizes):
    where = {}
    for a in reversed(axes):
        where[a] = k % sizes[a]
        k = k // sizes[a]
    return where


def tile_kernel(side_ref, places_ref, after_ref, tile_ref, cols_ref, d0, d1, t0, t1, sems, *, sizes):
    here = {a: lax.axis_index(a) for a in BLK}
    own = places_ref.shape[2]
    groups = tile_ref.shape[0]
    width = tile_ref.shape[3]
    turns = side_ref[6:7, 0:1]
    for b in range(width // own):
        block = block_at({**here, **unravel(b, REDUCE, sizes)}, sizes)
        cols_ref[:, b * own : (b + 1) * own] = features(places_ref[block], True).astype(jnp.bfloat16)

    def distances(c, d_ref):
        block = block_at({**here, **unravel(c, GATHER, sizes)}, sizes)
        psi = jnp.transpose(features(places_ref[block], False)).astype(jnp.bfloat16)
        d_ref[...] = dot(psi, cols_ref[...])

    def tile(d_ref, t_ref):
        for r in range(0, own, 16):
            for w in range(0, width, 512):
                real, imag = green_parts(d_ref[r : r + 16, w : w + 512], turns)
                t_ref[0, r : r + 16, w : w + 512] = real.astype(jnp.bfloat16)
                t_ref[1, r : r + 16, w : w + 512] = imag.astype(jnp.bfloat16)

    def out(c, t_ref, s):
        half = own // 2
        return [
            pltpu.make_async_copy(
                t_ref.at[p, h * half : (h + 1) * half], tile_ref.at[c, p, h * half : (h + 1) * half], sems.at[s, p, h]
            )
            for p in range(2)
            for h in range(2)
        ]

    distances(0, d0)

    def pair(k, carry):
        @pl.when(k > 0)
        def _():
            for copy in out(2 * k - 2, t0, 0):
                copy.wait()

        distances(2 * k + 1, d1)
        tile(d0, t0)
        for copy in out(2 * k, t0, 0):
            copy.start()

        @pl.when(k > 0)
        def _():
            for copy in out(2 * k - 1, t1, 1):
                copy.wait()

        distances(jnp.minimum(2 * k + 2, groups - 1), d0)
        tile(d1, t1)
        for copy in out(2 * k + 1, t1, 1):
            copy.start()
        return carry

    lax.fori_loop(0, groups // 2, pair, 0)
    for copy in out(groups - 2, t0, 0) + out(groups - 1, t1, 1):
        copy.wait()


def second_kernel(source_ref, tile_ref, part_ref, lhs_ref, all_ref, acc_r, acc_i, sems, *, node_count):
    groups, _, emitters, own = source_ref.shape
    targets = part_ref.shape[0]
    pieces = sems.shape[0]
    per = groups // pieces

    def bring(p):
        at = pl.ds(p * per, per)
        return pltpu.make_async_copy(tile_ref.at[at], all_ref.at[at], sems.at[p])

    for p in range(pieces):
        bring(p).start()
    for c in range(groups):
        lhs_ref[:, c * own : (c + 1) * own] = source_ref[c].reshape(2 * emitters, own)
    for p in range(pieces):
        bring(p).wait()
        lhs = lhs_ref[:, p * per * own : (p + 1) * per * own]
        for part, acc in ((0, acc_r), (1, acc_i)):
            rhs = all_ref[p * per : (p + 1) * per, part].reshape(per * own, targets * own)
            here = dot(lhs, rhs)
            acc[...] = here if p == 0 else acc[...] + here
    scale = GRID * float(node_count) ** (-0.5)
    for b in range(targets):
        at = slice(b * own, (b + 1) * own)
        part_ref[b, 0] = ((acc_r[0:emitters, at] - acc_i[emitters:, at]) * scale).astype(part_ref.dtype)
        part_ref[b, 1] = ((acc_r[emitters:, at] + acc_i[0:emitters, at]) * scale).astype(part_ref.dtype)


def last_kernel(parts_ref, first_ref, second_ref, terms_ref, *, share):
    real = parts_ref[0, 0].astype(jnp.float32)
    imag = parts_ref[0, 1].astype(jnp.float32)
    for b in range(1, parts_ref.shape[0]):
        real += parts_ref[b, 0].astype(jnp.float32)
        imag += parts_ref[b, 1].astype(jnp.float32)
    second_ref[0, 0] = real.astype(jnp.bfloat16)
    second_ref[0, 1] = imag.astype(jnp.bfloat16)
    terms = jnp.sum(first_ref[0] * real - first_ref[1] * imag, axis=0, keepdims=True) * share
    terms_ref[...] = jnp.broadcast_to(terms[None], terms_ref.shape)


VMEM = pl.BlockSpec(memory_space=pltpu.VMEM)
HBM = pl.BlockSpec(memory_space=pltpu.HBM)
SMEM = pl.BlockSpec(memory_space=pltpu.SMEM)


def limit(mib):
    return pltpu.CompilerParams(vmem_limit_bytes=mib << 20)


def local(node_index, emitters, admittance, wavenumbers):
    sizes = {a: lax.axis_size(a) for a in BLK}
    blocks = math.prod(sizes.values())
    lanes = lax.axis_size("freq")
    own = node_index.shape[1]
    count = blocks * own
    tx = emitters.shape[0]
    near, far = lax.axis_size(GATHER), lax.axis_size(REDUCE)

    f32, bf16 = jnp.float32, jnp.bfloat16
    copies = jnp.broadcast_to(node_index.astype(bf16), (blocks, *node_index.shape))
    places = lax.all_to_all(copies, BLK, split_axis=0, concat_axis=0, tiled=True)
    own_features, index, side = pl.pallas_call(
        start_kernel,
        out_shape=(
            jax.ShapeDtypeStruct((FEATURES, own), bf16),
            jax.ShapeDtypeStruct((tx, LANES), jnp.int32),
            jax.ShapeDtypeStruct((8, own), f32),
        ),
        in_specs=[SMEM, VMEM, VMEM, VMEM],
        out_specs=(VMEM,) * 3,
        compiler_params=limit(4),
        name="start",
    )(wavenumbers, node_index, emitters[None], admittance)
    width = 16 * own
    first, weighted = pl.pallas_call(
        first_kernel,
        out_shape=(
            jax.ShapeDtypeStruct((2, tx, own), f32),
            jax.ShapeDtypeStruct((near, 2, tx, own), bf16),
        ),
        in_specs=[VMEM] * 4,
        out_specs=(VMEM, VMEM),
        scratch_shapes=[
            pltpu.VMEM((own + tx, LANES), bf16),
            pltpu.VMEM((own + tx, width), f32),
            pltpu.VMEM((own + tx, width), f32),
            pltpu.VMEM((2 * (own + tx), width), bf16),
            pltpu.VMEM((2 * (own + tx), width), bf16),
            pltpu.VMEM((2 * tx, 2 * own), f32),
        ],
        compiler_params=limit(12),
        name="first_wave",
    )(side, places, own_features, index)

    source = lax.all_to_all(weighted, GATHER, split_axis=0, concat_axis=0, tiled=True)
    tile = pl.pallas_call(
        functools.partial(tile_kernel, sizes=sizes),
        out_shape=jax.ShapeDtypeStruct((near, 2, own, far * own), bf16),
        in_specs=[VMEM, VMEM, pl.BlockSpec(memory_space=pl.ANY)],
        out_specs=HBM,
        scratch_shapes=[
            pltpu.VMEM((FEATURES, far * own), bf16),
            pltpu.VMEM((own, far * own), f32),
            pltpu.VMEM((own, far * own), f32),
            pltpu.VMEM((2, own, far * own), bf16),
            pltpu.VMEM((2, own, far * own), bf16),
            pltpu.SemaphoreType.DMA((2, 2, 2)),
        ],
        compiler_params=limit(50),
        cost_estimate=pl.CostEstimate(flops=10**10, bytes_accessed=1 << 23, transcendentals=1 << 21),
        name="green_tile",
    )(side, places, first)
    part = pl.pallas_call(
        functools.partial(second_kernel, node_count=count),
        out_shape=jax.ShapeDtypeStruct((far, 2, tx, own), bf16),
        in_specs=[VMEM, HBM],
        out_specs=VMEM,
        scratch_shapes=[
            pltpu.VMEM((2 * tx, near * own), bf16),
            pltpu.VMEM((near, 2, own, far * own), bf16),
            pltpu.VMEM((2 * tx, far * own), f32),
            pltpu.VMEM((2 * tx, far * own), f32),
            pltpu.SemaphoreType.DMA((8,)),
        ],
        compiler_params=limit(50),
        name="second_wave",
    )(source, tile)
    parts = lax.all_to_all(part, REDUCE, split_axis=0, concat_axis=0, tiled=True)
    second, terms = pl.pallas_call(
        functools.partial(last_kernel, share=1.0 / (lanes * tx)),
        out_shape=(
            jax.ShapeDtypeStruct((1, 2, tx, own), bf16),
            jax.ShapeDtypeStruct((lanes, 1, own), f32),
        ),
        in_specs=[VMEM, VMEM],
        out_specs=(VMEM, VMEM),
        compiler_params=limit(4),
        name="last_sum",
    )(parts, first)
    terms = lax.all_to_all(terms, "freq", split_axis=0, concat_axis=0, tiled=True)
    return second, terms.sum(axis=(0, 1))


def solution(mesh):
    split = Mesh(mesh.devices.reshape(2, 2, 8, 4, mesh.shape["freq"]), (*BLK, "freq"))
    in_specs = (P(None, BLK), P(), P(None, BLK), P("freq"))
    out_specs = (P("freq", None, None, BLK), P(BLK))
    return jax.shard_map(local, mesh=split, in_specs=in_specs, out_specs=out_specs, check_vma=False)
```

```python
import functools
import math

import jax
import jax.numpy as jnp
from jax import lax
from jax.experimental import pallas as pl
from jax.experimental.pallas import tpu as pltpu
from jax.sharding import Mesh
from jax.sharding import PartitionSpec as P

GRID = 64
BLK = ("zs", "za", "y", "x")
GATHER = ("zs", "y")
REDUCE = ("za", "x")
LANES = 128
FEATURES = 16
SOFT = 0.0025 * GRID * GRID
MAGIC = 12582912.0
KEPT = 6
ROOT2 = math.sqrt(2.0)
SIN_POLY = [ROOT2 * c for c in (3.1415820221197075, -5.167142794757069, 2.541899010399708, -0.554636148527055)]
COS_POLY = [ROOT2 * c for c in (0.9999933001981278, -4.933938170377516, 4.04128504935244, -1.2221298133692595)]


def poly(coefs, s):
    total = coefs[-1] * s + coefs[-2]
    for c in coefs[-3::-1]:
        total = total * s + c
    return total


def green_parts(square, turns_per_step):
    v = square + SOFT
    inv = lax.rsqrt(v)
    turns = (v * inv) * turns_per_step
    f = turns - ((turns + MAGIC) - MAGIC)
    s = f * f
    half_sin = poly(SIN_POLY, s) * f
    half_cos = poly(COS_POLY, s)
    q = inv * half_sin
    return inv - q * half_sin, q * half_cos


def split_norm(p):
    n = jnp.sum(p * p, axis=0, keepdims=True)
    high = ((n * (1 / 64) + MAGIC) - MAGIC) * 64.0
    return high, n - high


def features(places, target):
    p = places.astype(jnp.float32) - 32.0
    high, low = split_norm(p)
    one = jnp.ones_like(high)
    zero = jnp.zeros((FEATURES - 7, p.shape[1]), jnp.float32)
    if target:
        return jnp.concatenate([p, high, low, one, one, zero], axis=0)
    return jnp.concatenate([p * -2.0, one, one, high, low, zero], axis=0)


def spread_features(x, y, z):
    lane = lax.broadcasted_iota(jnp.int32, x.shape, 1)
    x, y, z = x - 32.0, y - 32.0, z - 32.0
    n = x * x + y * y + z * z
    high = ((n * (1 / 64) + MAGIC) - MAGIC) * 64.0
    low = n - high
    out = jnp.where(lane == 0, x, 0.0)
    out = jnp.where(lane == 1, y, out)
    out = jnp.where(lane == 2, z, out)
    out = jnp.where(lane == 3, high, out)
    out = jnp.where(lane == 4, low, out)
    return jnp.where((lane == 5) | (lane == 6), 1.0, out)


def dot(a, b, contract=((1,), (0,))):
    return lax.dot_general(a, b, (contract, ((), ())), preferred_element_type=jnp.float32)


def copies_kernel(node_ref, copies_ref):
    places = node_ref[...].astype(jnp.float32).astype(jnp.bfloat16)
    copies_ref[...] = jnp.broadcast_to(places[None], copies_ref.shape)


def start_kernel(wavenumber_ref, node_ref, emitters_ref, admittance_ref, own_ref, index_ref, side_ref):
    own_ref[...] = features(node_ref[...], True).astype(jnp.bfloat16)
    emitters = jnp.broadcast_to(emitters_ref[...].astype(jnp.float32), (LANES, emitters_ref.shape[1]))
    index_ref[...] = jnp.transpose(emitters).astype(jnp.int32)
    side_ref[0:2] = admittance_ref[...]
    turns = wavenumber_ref[0] * (1.0 / (GRID * 2.0 * math.pi))
    side_ref[2:8] = jnp.full((6, side_ref.shape[1]), turns, jnp.float32)


def first_kernel(side_ref, places_ref, own_ref, index_ref, first_ref, weighted_ref,
                 rows_ref, d0, d1, g0, g1, acc_ref):
    blocks = places_ref.shape[0]
    own = own_ref.shape[1]
    emitters = index_ref.shape[0]
    width = d0.shape[1]
    per = width // own
    chunks = blocks // per
    turns = side_ref[6:7, 0:1]

    rows_ref[0:own, 0:FEATURES] = jnp.transpose(own_ref[...].astype(jnp.float32)).astype(jnp.bfloat16)
    index = index_ref[...]
    lane = lax.broadcasted_iota(jnp.int32, (emitters, LANES), 1)
    of_block = jnp.where(lane == index // own, 1.0, 0.0).astype(jnp.bfloat16)
    at_lane = lane == index % own
    every = jnp.ones((LANES, LANES), jnp.bfloat16)
    found = []
    for d in range(3):
        line = dot(of_block, places_ref[:, d, :])
        found.append(dot(jnp.where(at_lane, line, 0.0).astype(jnp.bfloat16), every))
    rows_ref[own : own + emitters] = spread_features(*found).astype(jnp.bfloat16)

    acc_ref[...] = jnp.zeros_like(acc_ref)

    def distances(chunk, d_ref):
        for b in range(per):
            psi = features(places_ref[chunk * per + b], False).astype(jnp.bfloat16)
            d_ref[:, b * own : (b + 1) * own] = dot(rows_ref[:, 0:FEATURES], psi)

    def tile(d_ref, g_ref):
        for r in range(0, own + emitters, 16):
            at = r if r < own else r + own
            step = own if r < own else emitters
            for w in range(0, width, 512):
                real, imag = green_parts(d_ref[r : r + 16, w : w + 512], turns)
                g_ref[at : at + 16, w : w + 512] = real.astype(jnp.bfloat16)
                g_ref[at + step : at + step + 16, w : w + 512] = imag.astype(jnp.bfloat16)

    def gather(g_ref):
        acc_ref[...] += dot(g_ref[2 * own :, :], g_ref[0 : 2 * own, :], ((1,), (1,)))

    distances(0, d0)
    g1[...] = jnp.zeros_like(g1)

    def pair(i, carry):
        distances(2 * i + 1, d1)
        tile(d0, g0)
        gather(g1)
        distances(jnp.minimum(2 * i + 2, chunks - 1), d0)
        tile(d1, g1)
        gather(g0)
        return carry

    lax.fori_loop(0, chunks // 2, pair, 0)
    gather(g1)
    scale = (GRID * GRID) * float(blocks * own) ** (-0.5)
    top, low = acc_ref[0:emitters, :], acc_ref[emitters:, :]
    real = (top[:, 0:own] - low[:, own:]) * scale
    imag = (low[:, 0:own] + top[:, own:]) * scale
    first_ref[0] = real
    first_ref[1] = imag
    a, b = side_ref[0:1, :], side_ref[1:2, :]
    w_real = (a * real - b * imag).astype(jnp.bfloat16)
    w_imag = (a * imag + b * real).astype(jnp.bfloat16)
    for k in range(weighted_ref.shape[0]):
        weighted_ref[k, 0] = w_real
        weighted_ref[k, 1] = w_imag


def block_at(where, sizes):
    place = 0
    for a in BLK:
        place = place * sizes[a] + where[a]
    return place


def unravel(k, axes, sizes):
    where = {}
    for a in reversed(axes):
        where[a] = k % sizes[a]
        k = k // sizes[a]
    return where


def tile_kernel(side_ref, places_ref, after_ref, tile_ref, near_ref, cols_ref, d0, d1, t0, t1, sems, *, sizes):
    here = {a: lax.axis_index(a) for a in BLK}
    own = places_ref.shape[2]
    far = tile_ref.shape[0]
    groups = far + near_ref.shape[0]
    width = tile_ref.shape[3]
    turns = side_ref[6:7, 0:1]
    for b in range(width // own):
        block = block_at({**here, **unravel(b, REDUCE, sizes)}, sizes)
        cols_ref[:, b * own : (b + 1) * own] = features(places_ref[block], True).astype(jnp.bfloat16)

    def distances(c, d_ref):
        block = block_at({**here, **unravel(c, GATHER, sizes)}, sizes)
        psi = jnp.transpose(features(places_ref[block], False)).astype(jnp.bfloat16)
        d_ref[...] = dot(psi, cols_ref[...])

    def tile(d_ref, store):
        for r in range(0, own, 16):
            for w in range(0, width, 512):
                real, imag = green_parts(d_ref[r : r + 16, w : w + 512], turns)
                store(0, r, w, real.astype(jnp.bfloat16))
                store(1, r, w, imag.astype(jnp.bfloat16))

    def into(t_ref):
        def store(p, r, w, value):
            t_ref[p, r : r + 16, w : w + 512] = value

        return store

    def kept(c):
        def store(p, r, w, value):
            near_ref[c, p, r : r + 16, w : w + 512] = value

        return store

    def out(c, t_ref, s):
        half = own // 2
        return [
            pltpu.make_async_copy(
                t_ref.at[p, h * half : (h + 1) * half], tile_ref.at[c, p, h * half : (h + 1) * half], sems.at[s, p, h]
            )
            for p in range(2)
            for h in range(2)
        ]

    distances(0, d0)

    def pair(k, carry):
        @pl.when(k > 0)
        def _():
            for copy in out(2 * k - 2, t0, 0):
                copy.wait()

        distances(2 * k + 1, d1)
        tile(d0, into(t0))
        for copy in out(2 * k, t0, 0):
            copy.start()

        @pl.when(k > 0)
        def _():
            for copy in out(2 * k - 1, t1, 1):
                copy.wait()

        distances(jnp.minimum(2 * k + 2, groups - 1), d0)
        tile(d1, into(t1))
        for copy in out(2 * k + 1, t1, 1):
            copy.start()
        return carry

    lax.fori_loop(0, far // 2, pair, 0)

    def last(k, carry):
        distances(far + 2 * k + 1, d1)
        tile(d0, kept(2 * k))
        distances(jnp.minimum(far + 2 * k + 2, groups - 1), d0)
        tile(d1, kept(2 * k + 1))
        return carry

    lax.fori_loop(0, (groups - far) // 2, last, 0)
    for copy in out(far - 2, t0, 0) + out(far - 1, t1, 1):
        copy.wait()


def second_kernel(source_ref, tile_ref, near_ref, part_ref, lhs_ref, all_ref, acc_r, acc_i, sems, *, node_count):
    groups, _, emitters, own = source_ref.shape
    targets = part_ref.shape[0]
    far = tile_ref.shape[0]
    per = far // sems.shape[0]

    def bring(p):
        at = pl.ds(p * per, per)
        return pltpu.make_async_copy(tile_ref.at[at], all_ref.at[at], sems.at[p])

    for p in range(far // per):
        bring(p).start()
    for c in range(groups):
        lhs_ref[:, c * own : (c + 1) * own] = source_ref[c].reshape(2 * emitters, own)
    for begin in [*range(far, groups, per), *range(0, far, per)]:
        if begin < far:
            bring(begin // per).wait()
        lhs = lhs_ref[:, begin * own : (begin + per) * own]
        for part, acc in ((0, acc_r), (1, acc_i)):
            held = all_ref[begin : begin + per] if begin < far else near_ref[begin - far : begin - far + per]
            here = dot(lhs, held[:, part].reshape(per * own, targets * own))
            acc[...] = here if begin == far else acc[...] + here
    scale = GRID * float(node_count) ** (-0.5)
    for b in range(targets):
        at = slice(b * own, (b + 1) * own)
        part_ref[b, 0] = ((acc_r[0:emitters, at] - acc_i[emitters:, at]) * scale).astype(part_ref.dtype)
        part_ref[b, 1] = ((acc_r[emitters:, at] + acc_i[0:emitters, at]) * scale).astype(part_ref.dtype)


def last_kernel(parts_ref, first_ref, second_ref, terms_ref, *, share):
    real = parts_ref[0, 0].astype(jnp.float32)
    imag = parts_ref[0, 1].astype(jnp.float32)
    for b in range(1, parts_ref.shape[0]):
        real += parts_ref[b, 0].astype(jnp.float32)
        imag += parts_ref[b, 1].astype(jnp.float32)
    second_ref[0, 0] = real.astype(jnp.bfloat16)
    second_ref[0, 1] = imag.astype(jnp.bfloat16)
    terms = jnp.sum(first_ref[0] * real - first_ref[1] * imag, axis=0, keepdims=True) * share
    terms_ref[...] = jnp.broadcast_to(terms[None], terms_ref.shape)


VMEM = pl.BlockSpec(memory_space=pltpu.VMEM)
HBM = pl.BlockSpec(memory_space=pltpu.HBM)
SMEM = pl.BlockSpec(memory_space=pltpu.SMEM)


def limit(mib):
    return pltpu.CompilerParams(vmem_limit_bytes=mib << 20)


def local(node_index, emitters, admittance, wavenumbers):
    sizes = {a: lax.axis_size(a) for a in BLK}
    blocks = math.prod(sizes.values())
    lanes = lax.axis_size("freq")
    own = node_index.shape[1]
    count = blocks * own
    tx = emitters.shape[0]
    near, far = lax.axis_size(GATHER), lax.axis_size(REDUCE)

    f32, bf16 = jnp.float32, jnp.bfloat16
    copies = pl.pallas_call(
        copies_kernel,
        out_shape=jax.ShapeDtypeStruct((blocks, *node_index.shape), bf16),
        in_specs=[VMEM],
        out_specs=VMEM,
        compiler_params=limit(60),
        name="copies",
    )(node_index)
    places = lax.all_to_all(copies, BLK, split_axis=0, concat_axis=0, tiled=True)
    own_features, index, side = pl.pallas_call(
        start_kernel,
        out_shape=(
            jax.ShapeDtypeStruct((FEATURES, own), bf16),
            jax.ShapeDtypeStruct((tx, LANES), jnp.int32),
            jax.ShapeDtypeStruct((8, own), f32),
        ),
        in_specs=[SMEM, VMEM, VMEM, VMEM],
        out_specs=(VMEM,) * 3,
        compiler_params=limit(4),
        name="start",
    )(wavenumbers, node_index, emitters[None], admittance)
    width = 16 * own
    first, weighted = pl.pallas_call(
        first_kernel,
        out_shape=(
            jax.ShapeDtypeStruct((2, tx, own), f32),
            jax.ShapeDtypeStruct((near, 2, tx, own), bf16),
        ),
        in_specs=[VMEM] * 4,
        out_specs=(VMEM, VMEM),
        scratch_shapes=[
            pltpu.VMEM((own + tx, LANES), bf16),
            pltpu.VMEM((own + tx, width), f32),
            pltpu.VMEM((own + tx, width), f32),
            pltpu.VMEM((2 * (own + tx), width), bf16),
            pltpu.VMEM((2 * (own + tx), width), bf16),
            pltpu.VMEM((2 * tx, 2 * own), f32),
        ],
        compiler_params=limit(12),
        name="first_wave",
    )(side, places, own_features, index)

    source = lax.all_to_all(weighted, GATHER, split_axis=0, concat_axis=0, tiled=True)
    kept = KEPT
    tile, tile_near = pl.pallas_call(
        functools.partial(tile_kernel, sizes=sizes),
        out_shape=(
            jax.ShapeDtypeStruct((near - kept, 2, own, far * own), bf16),
            jax.ShapeDtypeStruct((kept, 2, own, far * own), bf16),
        ),
        in_specs=[VMEM, VMEM, pl.BlockSpec(memory_space=pl.ANY)],
        out_specs=(HBM, VMEM),
        scratch_shapes=[
            pltpu.VMEM((FEATURES, far * own), bf16),
            pltpu.VMEM((own, far * own), f32),
            pltpu.VMEM((own, far * own), f32),
            pltpu.VMEM((2, own, far * own), bf16),
            pltpu.VMEM((2, own, far * own), bf16),
            pltpu.SemaphoreType.DMA((2, 2, 2)),
        ],
        compiler_params=limit(50),
        cost_estimate=pl.CostEstimate(flops=10**10, bytes_accessed=1 << 23, transcendentals=1 << 21),
        name="green_tile",
    )(side, places, first)
    part = pl.pallas_call(
        functools.partial(second_kernel, node_count=count),
        out_shape=jax.ShapeDtypeStruct((far, 2, tx, own), bf16),
        in_specs=[VMEM, HBM, VMEM],
        out_specs=VMEM,
        scratch_shapes=[
            pltpu.VMEM((2 * tx, near * own), bf16),
            pltpu.VMEM((near - kept, 2, own, far * own), bf16),
            pltpu.VMEM((2 * tx, far * own), f32),
            pltpu.VMEM((2 * tx, far * own), f32),
            pltpu.SemaphoreType.DMA(((near - kept) // 2,)),
        ],
        compiler_params=limit(50),
        name="second_wave",
    )(source, tile, tile_near)
    parts = lax.all_to_all(part, REDUCE, split_axis=0, concat_axis=0, tiled=True)
    second, terms = pl.pallas_call(
        functools.partial(last_kernel, share=1.0 / (lanes * tx)),
        out_shape=(
            jax.ShapeDtypeStruct((1, 2, tx, own), bf16),
            jax.ShapeDtypeStruct((lanes, 1, own), f32),
        ),
        in_specs=[VMEM, VMEM],
        out_specs=(VMEM, VMEM),
        compiler_params=limit(4),
        name="last_sum",
    )(parts, first)
    terms = lax.all_to_all(terms, "freq", split_axis=0, concat_axis=0, tiled=True)
    return second, terms.sum(axis=(0, 1))


def solution(mesh):
    split = Mesh(mesh.devices.reshape(2, 2, 8, 4, mesh.shape["freq"]), (*BLK, "freq"))
    in_specs = (P(None, BLK), P(), P(None, BLK), P("freq"))
    out_specs = (P("freq", None, None, BLK), P(BLK))
    return jax.shard_map(local, mesh=split, in_specs=in_specs, out_specs=out_specs, check_vma=False)
```

```python
import functools
import math

import jax
import jax.numpy as jnp
from jax import lax
from jax.experimental import pallas as pl
from jax.experimental.pallas import tpu as pltpu
from jax.sharding import Mesh
from jax.sharding import PartitionSpec as P

GRID = 64
BLK = ("zs", "za", "y", "x")
GATHER = ("zs", "y")
REDUCE = ("za", "x")
LANES = 128
FEATURES = 16
SOFT = 0.0025 * GRID * GRID
MAGIC = 12582912.0
KEPT = 4
ROOT2 = math.sqrt(2.0)
SIN_POLY = [ROOT2 * c for c in (3.1415820221197075, -5.167142794757069, 2.541899010399708, -0.554636148527055)]
COS_POLY = [ROOT2 * c for c in (0.9999933001981278, -4.933938170377516, 4.04128504935244, -1.2221298133692595)]


def poly(coefs, s):
    total = coefs[-1] * s + coefs[-2]
    for c in coefs[-3::-1]:
        total = total * s + c
    return total


def green_parts(square, turns_per_step):
    v = square + SOFT
    inv = lax.rsqrt(v)
    turns = (v * inv) * turns_per_step
    f = turns - ((turns + MAGIC) - MAGIC)
    s = f * f
    half_sin = poly(SIN_POLY, s) * f
    half_cos = poly(COS_POLY, s)
    q = inv * half_sin
    return inv - q * half_sin, q * half_cos


def split_norm(p):
    n = jnp.sum(p * p, axis=0, keepdims=True)
    high = ((n * (1 / 64) + MAGIC) - MAGIC) * 64.0
    return high, n - high


def features(places, target):
    p = places.astype(jnp.float32) - 32.0
    high, low = split_norm(p)
    one = jnp.ones_like(high)
    zero = jnp.zeros((FEATURES - 7, p.shape[1]), jnp.float32)
    if target:
        return jnp.concatenate([p, high, low, one, one, zero], axis=0)
    return jnp.concatenate([p * -2.0, one, one, high, low, zero], axis=0)


def spread_features(x, y, z):
    lane = lax.broadcasted_iota(jnp.int32, x.shape, 1)
    x, y, z = x - 32.0, y - 32.0, z - 32.0
    n = x * x + y * y + z * z
    high = ((n * (1 / 64) + MAGIC) - MAGIC) * 64.0
    low = n - high
    out = jnp.where(lane == 0, x, 0.0)
    out = jnp.where(lane == 1, y, out)
    out = jnp.where(lane == 2, z, out)
    out = jnp.where(lane == 3, high, out)
    out = jnp.where(lane == 4, low, out)
    return jnp.where((lane == 5) | (lane == 6), 1.0, out)


def dot(a, b, contract=((1,), (0,))):
    return lax.dot_general(a, b, (contract, ((), ())), preferred_element_type=jnp.float32)


def start_kernel(wavenumber_ref, node_ref, emitters_ref, admittance_ref, own_ref, index_ref, side_ref):
    own_ref[...] = features(node_ref[...], True).astype(jnp.bfloat16)
    emitters = jnp.broadcast_to(emitters_ref[...].astype(jnp.float32), (LANES, emitters_ref.shape[1]))
    index_ref[...] = jnp.transpose(emitters).astype(jnp.int32)
    side_ref[0:2] = admittance_ref[...]
    turns = wavenumber_ref[0] * (1.0 / (GRID * 2.0 * math.pi))
    side_ref[2:8] = jnp.full((6, side_ref.shape[1]), turns, jnp.float32)


def first_kernel(side_ref, places_ref, own_ref, index_ref, first_ref, weighted_ref,
                 rows_ref, d0, d1, g0, g1, acc_ref):
    blocks = places_ref.shape[0]
    own = own_ref.shape[1]
    emitters = index_ref.shape[0]
    width = d0.shape[1]
    per = width // own
    chunks = blocks // per
    turns = side_ref[6:7, 0:1]

    rows_ref[0:own, 0:FEATURES] = jnp.transpose(own_ref[...].astype(jnp.float32)).astype(jnp.bfloat16)
    index = index_ref[...]
    lane = lax.broadcasted_iota(jnp.int32, (emitters, LANES), 1)
    of_block = jnp.where(lane == index // own, 1.0, 0.0).astype(jnp.bfloat16)
    at_lane = lane == index % own
    every = jnp.ones((LANES, LANES), jnp.bfloat16)
    found = []
    for d in range(3):
        line = dot(of_block, places_ref[:, d, :])
        found.append(dot(jnp.where(at_lane, line, 0.0).astype(jnp.bfloat16), every))
    rows_ref[own : own + emitters] = spread_features(*found).astype(jnp.bfloat16)

    acc_ref[...] = jnp.zeros_like(acc_ref)

    def distances(chunk, d_ref):
        for b in range(per):
            psi = features(places_ref[chunk * per + b], False).astype(jnp.bfloat16)
            d_ref[:, b * own : (b + 1) * own] = dot(rows_ref[:, 0:FEATURES], psi)

    def tile(d_ref, g_ref):
        for r in range(0, own + emitters, 16):
            at = r if r < own else r + own
            step = own if r < own else emitters
            for w in range(0, width, 512):
                real, imag = green_parts(d_ref[r : r + 16, w : w + 512], turns)
                g_ref[at : at + 16, w : w + 512] = real.astype(jnp.bfloat16)
                g_ref[at + step : at + step + 16, w : w + 512] = imag.astype(jnp.bfloat16)

    def gather(g_ref):
        acc_ref[...] += dot(g_ref[2 * own :, :], g_ref[0 : 2 * own, :], ((1,), (1,)))

    distances(0, d0)
    g1[...] = jnp.zeros_like(g1)

    def pair(i, carry):
        distances(2 * i + 1, d1)
        tile(d0, g0)
        gather(g1)
        distances(jnp.minimum(2 * i + 2, chunks - 1), d0)
        tile(d1, g1)
        gather(g0)
        return carry

    lax.fori_loop(0, chunks // 2, pair, 0)
    gather(g1)
    scale = (GRID * GRID) * float(blocks * own) ** (-0.5)
    top, low = acc_ref[0:emitters, :], acc_ref[emitters:, :]
    real = (top[:, 0:own] - low[:, own:]) * scale
    imag = (low[:, 0:own] + top[:, own:]) * scale
    first_ref[0] = real
    first_ref[1] = imag
    a, b = side_ref[0:1, :], side_ref[1:2, :]
    w_real = (a * real - b * imag).astype(jnp.bfloat16)
    w_imag = (a * imag + b * real).astype(jnp.bfloat16)
    for k in range(weighted_ref.shape[0]):
        weighted_ref[k, 0] = w_real
        weighted_ref[k, 1] = w_imag


def block_at(where, sizes):
    place = 0
    for a in BLK:
        place = place * sizes[a] + where[a]
    return place


def unravel(k, axes, sizes):
    where = {}
    for a in reversed(axes):
        where[a] = k % sizes[a]
        k = k // sizes[a]
    return where


def tile_kernel(side_ref, places_ref, after_ref, tile_ref, near_ref, cols_ref, d0, d1, t0, t1, sems, *, sizes):
    here = {a: lax.axis_index(a) for a in BLK}
    own = places_ref.shape[2]
    far = tile_ref.shape[0]
    groups = far + near_ref.shape[0]
    width = tile_ref.shape[3]
    turns = side_ref[6:7, 0:1]
    for b in range(width // own):
        block = block_at({**here, **unravel(b, REDUCE, sizes)}, sizes)
        cols_ref[:, b * own : (b + 1) * own] = features(places_ref[block], True).astype(jnp.bfloat16)

    def distances(c, d_ref):
        block = block_at({**here, **unravel(c, GATHER, sizes)}, sizes)
        psi = jnp.transpose(features(places_ref[block], False)).astype(jnp.bfloat16)
        d_ref[...] = dot(psi, cols_ref[...])

    def tile(d_ref, store):
        for r in range(0, own, 16):
            for w in range(0, width, 512):
                real, imag = green_parts(d_ref[r : r + 16, w : w + 512], turns)
                store(0, r, w, real.astype(jnp.bfloat16))
                store(1, r, w, imag.astype(jnp.bfloat16))

    def into(t_ref):
        def store(p, r, w, value):
            t_ref[p, r : r + 16, w : w + 512] = value

        return store

    def kept(c):
        def store(p, r, w, value):
            near_ref[c, p, r : r + 16, w : w + 512] = value

        return store

    def out(c, t_ref, s):
        half = own // 2
        return [
            pltpu.make_async_copy(
                t_ref.at[p, h * half : (h + 1) * half], tile_ref.at[c, p, h * half : (h + 1) * half], sems.at[s, p, h]
            )
            for p in range(2)
            for h in range(2)
        ]

    distances(0, d0)

    def pair(k, carry):
        @pl.when(k > 0)
        def _():
            for copy in out(2 * k - 2, t0, 0):
                copy.wait()

        distances(2 * k + 1, d1)
        tile(d0, into(t0))
        for copy in out(2 * k, t0, 0):
            copy.start()

        @pl.when(k > 0)
        def _():
            for copy in out(2 * k - 1, t1, 1):
                copy.wait()

        distances(jnp.minimum(2 * k + 2, groups - 1), d0)
        tile(d1, into(t1))
        for copy in out(2 * k + 1, t1, 1):
            copy.start()
        return carry

    lax.fori_loop(0, far // 2, pair, 0)

    def last(k, carry):
        distances(far + 2 * k + 1, d1)
        tile(d0, kept(2 * k))
        distances(jnp.minimum(far + 2 * k + 2, groups - 1), d0)
        tile(d1, kept(2 * k + 1))
        return carry

    lax.fori_loop(0, (groups - far) // 2, last, 0)
    for copy in out(far - 2, t0, 0) + out(far - 1, t1, 1):
        copy.wait()


def second_kernel(source_ref, tile_ref, near_ref, part_ref, lhs_ref, all_ref, acc_r, acc_i, sems, *, node_count):
    groups, _, emitters, own = source_ref.shape
    targets = part_ref.shape[0]
    far = tile_ref.shape[0]
    per = far // sems.shape[0]

    def bring(p):
        at = pl.ds(p * per, per)
        return pltpu.make_async_copy(tile_ref.at[at], all_ref.at[at], sems.at[p])

    for p in range(far // per):
        bring(p).start()
    for c in range(groups):
        lhs_ref[:, c * own : (c + 1) * own] = source_ref[c].reshape(2 * emitters, own)
    for begin, count in [(far, groups - far), *((p, per) for p in range(0, far, per))]:
        if begin < far:
            bring(begin // per).wait()
        lhs = lhs_ref[:, begin * own : (begin + count) * own]
        for part, acc in ((0, acc_r), (1, acc_i)):
            held = near_ref[:, part] if begin == far else all_ref[begin : begin + count, part]
            here = dot(lhs, held.reshape(count * own, targets * own))
            acc[...] = here if begin == far else acc[...] + here
    scale = GRID * float(node_count) ** (-0.5)
    for b in range(targets):
        at = slice(b * own, (b + 1) * own)
        part_ref[b, 0] = ((acc_r[0:emitters, at] - acc_i[emitters:, at]) * scale).astype(part_ref.dtype)
        part_ref[b, 1] = ((acc_r[emitters:, at] + acc_i[0:emitters, at]) * scale).astype(part_ref.dtype)


def last_kernel(parts_ref, first_ref, second_ref, terms_ref, *, share):
    real = parts_ref[0, 0].astype(jnp.float32)
    imag = parts_ref[0, 1].astype(jnp.float32)
    for b in range(1, parts_ref.shape[0]):
        real += parts_ref[b, 0].astype(jnp.float32)
        imag += parts_ref[b, 1].astype(jnp.float32)
    second_ref[0, 0] = real.astype(jnp.bfloat16)
    second_ref[0, 1] = imag.astype(jnp.bfloat16)
    terms = jnp.sum(first_ref[0] * real - first_ref[1] * imag, axis=0, keepdims=True) * share
    terms_ref[...] = jnp.broadcast_to(terms[None], terms_ref.shape)


VMEM = pl.BlockSpec(memory_space=pltpu.VMEM)
HBM = pl.BlockSpec(memory_space=pltpu.HBM)
SMEM = pl.BlockSpec(memory_space=pltpu.SMEM)


def limit(mib):
    return pltpu.CompilerParams(vmem_limit_bytes=mib << 20)


def local(node_index, emitters, admittance, wavenumbers):
    sizes = {a: lax.axis_size(a) for a in BLK}
    blocks = math.prod(sizes.values())
    lanes = lax.axis_size("freq")
    own = node_index.shape[1]
    count = blocks * own
    tx = emitters.shape[0]
    near, far = lax.axis_size(GATHER), lax.axis_size(REDUCE)

    f32, bf16 = jnp.float32, jnp.bfloat16
    copies = jnp.broadcast_to(node_index.astype(bf16), (blocks, *node_index.shape))
    places = lax.all_to_all(copies, BLK, split_axis=0, concat_axis=0, tiled=True)
    own_features, index, side = pl.pallas_call(
        start_kernel,
        out_shape=(
            jax.ShapeDtypeStruct((FEATURES, own), bf16),
            jax.ShapeDtypeStruct((tx, LANES), jnp.int32),
            jax.ShapeDtypeStruct((8, own), f32),
        ),
        in_specs=[SMEM, VMEM, VMEM, VMEM],
        out_specs=(VMEM,) * 3,
        compiler_params=limit(4),
        name="start",
    )(wavenumbers, node_index, emitters[None], admittance)
    width = 16 * own
    first, weighted = pl.pallas_call(
        first_kernel,
        out_shape=(
            jax.ShapeDtypeStruct((2, tx, own), f32),
            jax.ShapeDtypeStruct((near, 2, tx, own), bf16),
        ),
        in_specs=[VMEM] * 4,
        out_specs=(VMEM, VMEM),
        scratch_shapes=[
            pltpu.VMEM((own + tx, LANES), bf16),
            pltpu.VMEM((own + tx, width), f32),
            pltpu.VMEM((own + tx, width), f32),
            pltpu.VMEM((2 * (own + tx), width), bf16),
            pltpu.VMEM((2 * (own + tx), width), bf16),
            pltpu.VMEM((2 * tx, 2 * own), f32),
        ],
        compiler_params=limit(12),
        name="first_wave",
    )(side, places, own_features, index)

    source = lax.all_to_all(weighted, GATHER, split_axis=0, concat_axis=0, tiled=True)
    kept = KEPT
    tile, tile_near = pl.pallas_call(
        functools.partial(tile_kernel, sizes=sizes),
        out_shape=(
            jax.ShapeDtypeStruct((near - kept, 2, own, far * own), bf16),
            jax.ShapeDtypeStruct((kept, 2, own, far * own), bf16),
        ),
        in_specs=[VMEM, VMEM, pl.BlockSpec(memory_space=pl.ANY)],
        out_specs=(HBM, VMEM),
        scratch_shapes=[
            pltpu.VMEM((FEATURES, far * own), bf16),
            pltpu.VMEM((own, far * own), f32),
            pltpu.VMEM((own, far * own), f32),
            pltpu.VMEM((2, own, far * own), bf16),
            pltpu.VMEM((2, own, far * own), bf16),
            pltpu.SemaphoreType.DMA((2, 2, 2)),
        ],
        compiler_params=limit(50),
        cost_estimate=pl.CostEstimate(flops=10**10, bytes_accessed=1 << 23, transcendentals=1 << 21),
        name="green_tile",
    )(side, places, first)
    part = pl.pallas_call(
        functools.partial(second_kernel, node_count=count),
        out_shape=jax.ShapeDtypeStruct((far, 2, tx, own), bf16),
        in_specs=[VMEM, HBM, VMEM],
        out_specs=VMEM,
        scratch_shapes=[
            pltpu.VMEM((2 * tx, near * own), bf16),
            pltpu.VMEM((near - kept, 2, own, far * own), bf16),
            pltpu.VMEM((2 * tx, far * own), f32),
            pltpu.VMEM((2 * tx, far * own), f32),
            pltpu.SemaphoreType.DMA((3,)),
        ],
        compiler_params=limit(50),
        name="second_wave",
    )(source, tile, tile_near)
    parts = lax.all_to_all(part, REDUCE, split_axis=0, concat_axis=0, tiled=True)
    second, terms = pl.pallas_call(
        functools.partial(last_kernel, share=1.0 / (lanes * tx)),
        out_shape=(
            jax.ShapeDtypeStruct((1, 2, tx, own), bf16),
            jax.ShapeDtypeStruct((lanes, 1, own), f32),
        ),
        in_specs=[VMEM, VMEM],
        out_specs=(VMEM, VMEM),
        compiler_params=limit(4),
        name="last_sum",
    )(parts, first)
    terms = lax.all_to_all(terms, "freq", split_axis=0, concat_axis=0, tiled=True)
    return second, terms.sum(axis=(0, 1))


def solution(mesh):
    split = Mesh(mesh.devices.reshape(2, 2, 8, 4, mesh.shape["freq"]), (*BLK, "freq"))
    in_specs = (P(None, BLK), P(), P(None, BLK), P("freq"))
    out_specs = (P("freq", None, None, BLK), P(BLK))
    return jax.shard_map(local, mesh=split, in_specs=in_specs, out_specs=out_specs, check_vma=False)
```

```python
import functools
import math

import jax
import jax.numpy as jnp
from jax import lax
from jax.experimental import pallas as pl
from jax.experimental.pallas import tpu as pltpu
from jax.sharding import Mesh
from jax.sharding import PartitionSpec as P

GRID = 64
BLK = ("zs", "za", "y", "x")
GATHER = ("zs", "y")
REDUCE = ("za", "x")
LANES = 128
FEATURES = 16
SOFT = 0.0025 * GRID * GRID


def bf16_parts(x, count):
    parts = []
    for _ in range(count):
        mantissa, exponent = math.frexp(x)
        parts.append(math.ldexp(round(mantissa * 256), exponent - 8))
        x -= parts[-1]
    return parts


SOFT_PARTS = bf16_parts(SOFT, 3)
MAGIC = 12582912.0
KEPT = 4
ROOT2 = math.sqrt(2.0)
SIN_POLY = [ROOT2 * c for c in (3.1415820221197075, -5.167142794757069, 2.541899010399708, -0.554636148527055)]
COS_POLY = [ROOT2 * c for c in (0.9999933001981278, -4.933938170377516, 4.04128504935244, -1.2221298133692595)]


def poly(coefs, s):
    total = coefs[-1] * s + coefs[-2]
    for c in coefs[-3::-1]:
        total = total * s + c
    return total


def green_parts(v, turns_per_step):
    inv = lax.rsqrt(v)
    turns = (v * inv) * turns_per_step
    f = turns - lax.round(turns, lax.RoundingMethod.TO_NEAREST_EVEN)
    s = f * f
    half_sin = poly(SIN_POLY, s) * f
    half_cos = poly(COS_POLY, s)
    q = inv * half_sin
    return inv - q * half_sin, q * half_cos


def split_norm(p):
    n = jnp.sum(p * p, axis=0, keepdims=True)
    high = ((n * (1 / 64) + MAGIC) - MAGIC) * 64.0
    return high, n - high


def features(places, target):
    p = places.astype(jnp.float32) - 32.0
    high, low = split_norm(p)
    one = jnp.ones_like(high)
    zero = jnp.zeros((FEATURES - 7 - len(SOFT_PARTS), p.shape[1]), jnp.float32)
    if target:
        return jnp.concatenate([p, high, low, *[one] * (2 + len(SOFT_PARTS)), zero], axis=0)
    soft = [jnp.full_like(one, c) for c in SOFT_PARTS]
    return jnp.concatenate([p * -2.0, one, one, high, low, *soft, zero], axis=0)


def spread_features(x, y, z):
    lane = lax.broadcasted_iota(jnp.int32, x.shape, 1)
    x, y, z = x - 32.0, y - 32.0, z - 32.0
    n = x * x + y * y + z * z
    high = ((n * (1 / 64) + MAGIC) - MAGIC) * 64.0
    low = n - high
    out = jnp.where(lane == 0, x, 0.0)
    out = jnp.where(lane == 1, y, out)
    out = jnp.where(lane == 2, z, out)
    out = jnp.where(lane == 3, high, out)
    out = jnp.where(lane == 4, low, out)
    return jnp.where((lane >= 5) & (lane < 7 + len(SOFT_PARTS)), 1.0, out)


def dot(a, b, contract=((1,), (0,))):
    return lax.dot_general(a, b, (contract, ((), ())), preferred_element_type=jnp.float32)


def start_kernel(wavenumber_ref, node_ref, emitters_ref, admittance_ref, own_ref, index_ref, side_ref):
    own_ref[...] = features(node_ref[...], True).astype(jnp.bfloat16)
    emitters = jnp.broadcast_to(emitters_ref[...].astype(jnp.float32), (LANES, emitters_ref.shape[1]))
    index_ref[...] = jnp.transpose(emitters).astype(jnp.int32)
    side_ref[0:2] = admittance_ref[...]
    turns = wavenumber_ref[0] * (1.0 / (GRID * 2.0 * math.pi))
    side_ref[2:8] = jnp.full((6, side_ref.shape[1]), turns, jnp.float32)


def first_kernel(side_ref, places_ref, own_ref, index_ref, first_ref, weighted_ref,
                 rows_ref, c0, c1, g0, g1, acc_ref):
    blocks = places_ref.shape[0]
    own = own_ref.shape[1]
    emitters = index_ref.shape[0]
    width = c0.shape[1]
    per = width // own
    chunks = blocks // per
    turns = side_ref[6:7, 0:1]

    rows_ref[0:own, 0:FEATURES] = jnp.transpose(own_ref[...].astype(jnp.float32)).astype(jnp.bfloat16)
    index = index_ref[...]
    lane = lax.broadcasted_iota(jnp.int32, (emitters, LANES), 1)
    of_block = jnp.where(lane == index // own, 1.0, 0.0).astype(jnp.bfloat16)
    at_lane = lane == index % own
    every = jnp.ones((LANES, LANES), jnp.bfloat16)
    found = []
    for d in range(3):
        line = dot(of_block, places_ref[:, d, :])
        found.append(dot(jnp.where(at_lane, line, 0.0).astype(jnp.bfloat16), every))
    rows_ref[own : own + emitters] = spread_features(*found).astype(jnp.bfloat16)

    acc_ref[...] = jnp.zeros_like(acc_ref)

    def columns(chunk, c_ref):
        for b in range(per):
            psi = features(places_ref[chunk * per + b], False)
            c_ref[:, b * own : (b + 1) * own] = psi.astype(jnp.bfloat16)

    def tile(c_ref, g_ref):
        for w in range(0, width, 256):
            psi = c_ref[:, w : w + 256]
            for r in range(0, own + emitters, 64):
                at = r if r < own else r + own
                step = own if r < own else emitters
                real, imag = green_parts(dot(rows_ref[r : r + 64, 0:FEATURES], psi), turns)
                g_ref[at : at + 64, w : w + 256] = real.astype(jnp.bfloat16)
                g_ref[at + step : at + step + 64, w : w + 256] = imag.astype(jnp.bfloat16)

    def gather(g_ref):
        acc_ref[...] += dot(g_ref[2 * own :, :], g_ref[0 : 2 * own, :], ((1,), (1,)))

    columns(0, c0)
    g1[...] = jnp.zeros_like(g1)

    def pair(i, carry):
        columns(2 * i + 1, c1)
        tile(c0, g0)
        gather(g1)
        columns(jnp.minimum(2 * i + 2, chunks - 1), c0)
        tile(c1, g1)
        gather(g0)
        return carry

    lax.fori_loop(0, chunks // 2, pair, 0)
    gather(g1)
    scale = (GRID * GRID) * float(blocks * own) ** (-0.5)
    top, low = acc_ref[0:emitters, :], acc_ref[emitters:, :]
    real = (top[:, 0:own] - low[:, own:]) * scale
    imag = (low[:, 0:own] + top[:, own:]) * scale
    first_ref[0] = real
    first_ref[1] = imag
    a, b = side_ref[0:1, :], side_ref[1:2, :]
    w_real = (a * real - b * imag).astype(jnp.bfloat16)
    w_imag = (a * imag + b * real).astype(jnp.bfloat16)
    for k in range(weighted_ref.shape[0]):
        weighted_ref[k, 0] = w_real
        weighted_ref[k, 1] = w_imag


def block_at(where, sizes):
    place = 0
    for a in BLK:
        place = place * sizes[a] + where[a]
    return place


def unravel(k, axes, sizes):
    where = {}
    for a in reversed(axes):
        where[a] = k % sizes[a]
        k = k // sizes[a]
    return where


def tile_kernel(side_ref, places_ref, after_ref, tile_ref, near_ref, cols_ref, d0, d1, t0, t1, sems, *, sizes):
    here = {a: lax.axis_index(a) for a in BLK}
    own = places_ref.shape[2]
    far = tile_ref.shape[0]
    groups = far + near_ref.shape[0]
    width = tile_ref.shape[3]
    turns = side_ref[6:7, 0:1]
    for b in range(width // own):
        block = block_at({**here, **unravel(b, REDUCE, sizes)}, sizes)
        cols_ref[:, b * own : (b + 1) * own] = features(places_ref[block], True).astype(jnp.bfloat16)

    def distances(c, d_ref):
        block = block_at({**here, **unravel(c, GATHER, sizes)}, sizes)
        psi = jnp.transpose(features(places_ref[block], False)).astype(jnp.bfloat16)
        d_ref[...] = dot(psi, cols_ref[...])

    def tile(d_ref, store):
        for r in range(0, own, 16):
            for w in range(0, width, 512):
                real, imag = green_parts(d_ref[r : r + 16, w : w + 512], turns)
                store(0, r, w, real.astype(jnp.bfloat16))
                store(1, r, w, imag.astype(jnp.bfloat16))

    def into(t_ref):
        def store(p, r, w, value):
            t_ref[p, r : r + 16, w : w + 512] = value

        return store

    def kept(c):
        def store(p, r, w, value):
            near_ref[c, p, r : r + 16, w : w + 512] = value

        return store

    def out(c, t_ref, s):
        half = own // 2
        return [
            pltpu.make_async_copy(
                t_ref.at[p, h * half : (h + 1) * half], tile_ref.at[c, p, h * half : (h + 1) * half], sems.at[s, p, h]
            )
            for p in range(2)
            for h in range(2)
        ]

    distances(0, d0)

    def pair(k, carry):
        @pl.when(k > 0)
        def _():
            for copy in out(2 * k - 2, t0, 0):
                copy.wait()

        distances(2 * k + 1, d1)
        tile(d0, into(t0))
        for copy in out(2 * k, t0, 0):
            copy.start()

        @pl.when(k > 0)
        def _():
            for copy in out(2 * k - 1, t1, 1):
                copy.wait()

        distances(jnp.minimum(2 * k + 2, groups - 1), d0)
        tile(d1, into(t1))
        for copy in out(2 * k + 1, t1, 1):
            copy.start()
        return carry

    lax.fori_loop(0, far // 2, pair, 0)

    def last(k, carry):
        distances(far + 2 * k + 1, d1)
        tile(d0, kept(2 * k))
        distances(jnp.minimum(far + 2 * k + 2, groups - 1), d0)
        tile(d1, kept(2 * k + 1))
        return carry

    lax.fori_loop(0, (groups - far) // 2, last, 0)
    for copy in out(far - 2, t0, 0) + out(far - 1, t1, 1):
        copy.wait()


def second_kernel(source_ref, tile_ref, near_ref, part_ref, lhs_ref, all_ref, acc_r, acc_i, sems, *, node_count):
    groups, _, emitters, own = source_ref.shape
    targets = part_ref.shape[0]
    far = tile_ref.shape[0]
    per = far // sems.shape[0]

    def bring(p):
        at = pl.ds(p * per, per)
        return pltpu.make_async_copy(tile_ref.at[at], all_ref.at[at], sems.at[p])

    for p in range(far // per):
        bring(p).start()
    for c in range(groups):
        lhs_ref[:, c * own : (c + 1) * own] = source_ref[c].reshape(2 * emitters, own)
    for begin, count in [(far, groups - far), *((p, per) for p in range(0, far, per))]:
        if begin < far:
            bring(begin // per).wait()
        lhs = lhs_ref[:, begin * own : (begin + count) * own]
        for part, acc in ((0, acc_r), (1, acc_i)):
            held = near_ref[:, part] if begin == far else all_ref[begin : begin + count, part]
            here = dot(lhs, held.reshape(count * own, targets * own))
            acc[...] = here if begin == far else acc[...] + here
    scale = GRID * float(node_count) ** (-0.5)
    for b in range(targets):
        at = slice(b * own, (b + 1) * own)
        part_ref[b, 0] = ((acc_r[0:emitters, at] - acc_i[emitters:, at]) * scale).astype(part_ref.dtype)
        part_ref[b, 1] = ((acc_r[emitters:, at] + acc_i[0:emitters, at]) * scale).astype(part_ref.dtype)


def last_kernel(parts_ref, first_ref, second_ref, terms_ref, *, share):
    real = parts_ref[0, 0].astype(jnp.float32)
    imag = parts_ref[0, 1].astype(jnp.float32)
    for b in range(1, parts_ref.shape[0]):
        real += parts_ref[b, 0].astype(jnp.float32)
        imag += parts_ref[b, 1].astype(jnp.float32)
    second_ref[0, 0] = real.astype(jnp.bfloat16)
    second_ref[0, 1] = imag.astype(jnp.bfloat16)
    terms = jnp.sum(first_ref[0] * real - first_ref[1] * imag, axis=0, keepdims=True) * share
    terms_ref[...] = jnp.broadcast_to(terms[None], terms_ref.shape)


VMEM = pl.BlockSpec(memory_space=pltpu.VMEM)
HBM = pl.BlockSpec(memory_space=pltpu.HBM)
SMEM = pl.BlockSpec(memory_space=pltpu.SMEM)


def limit(mib):
    return pltpu.CompilerParams(vmem_limit_bytes=mib << 20)


def local(node_index, emitters, admittance, wavenumbers):
    sizes = {a: lax.axis_size(a) for a in BLK}
    blocks = math.prod(sizes.values())
    lanes = lax.axis_size("freq")
    own = node_index.shape[1]
    count = blocks * own
    tx = emitters.shape[0]
    near, far = lax.axis_size(GATHER), lax.axis_size(REDUCE)

    f32, bf16 = jnp.float32, jnp.bfloat16
    copies = jnp.broadcast_to(node_index.astype(bf16), (blocks, *node_index.shape))
    places = lax.all_to_all(copies, BLK, split_axis=0, concat_axis=0, tiled=True)
    own_features, index, side = pl.pallas_call(
        start_kernel,
        out_shape=(
            jax.ShapeDtypeStruct((FEATURES, own), bf16),
            jax.ShapeDtypeStruct((tx, LANES), jnp.int32),
            jax.ShapeDtypeStruct((8, own), f32),
        ),
        in_specs=[SMEM, VMEM, VMEM, VMEM],
        out_specs=(VMEM,) * 3,
        compiler_params=limit(4),
        name="start",
    )(wavenumbers, node_index, emitters[None], admittance)
    width = 16 * own
    first, weighted = pl.pallas_call(
        first_kernel,
        out_shape=(
            jax.ShapeDtypeStruct((2, tx, own), f32),
            jax.ShapeDtypeStruct((near, 2, tx, own), bf16),
        ),
        in_specs=[VMEM] * 4,
        out_specs=(VMEM, VMEM),
        scratch_shapes=[
            pltpu.VMEM((own + tx, LANES), bf16),
            pltpu.VMEM((FEATURES, width), bf16),
            pltpu.VMEM((FEATURES, width), bf16),
            pltpu.VMEM((2 * (own + tx), width), bf16),
            pltpu.VMEM((2 * (own + tx), width), bf16),
            pltpu.VMEM((2 * tx, 2 * own), f32),
        ],
        compiler_params=limit(12),
        name="first_wave",
    )(side, places, own_features, index)

    source = lax.all_to_all(weighted, GATHER, split_axis=0, concat_axis=0, tiled=True)
    kept = KEPT
    tile, tile_near = pl.pallas_call(
        functools.partial(tile_kernel, sizes=sizes),
        out_shape=(
            jax.ShapeDtypeStruct((near - kept, 2, own, far * own), bf16),
            jax.ShapeDtypeStruct((kept, 2, own, far * own), bf16),
        ),
        in_specs=[VMEM, VMEM, pl.BlockSpec(memory_space=pl.ANY)],
        out_specs=(HBM, VMEM),
        scratch_shapes=[
            pltpu.VMEM((FEATURES, far * own), bf16),
            pltpu.VMEM((own, far * own), f32),
            pltpu.VMEM((own, far * own), f32),
            pltpu.VMEM((2, own, far * own), bf16),
            pltpu.VMEM((2, own, far * own), bf16),
            pltpu.SemaphoreType.DMA((2, 2, 2)),
        ],
        compiler_params=limit(50),
        cost_estimate=pl.CostEstimate(flops=10**10, bytes_accessed=1 << 23, transcendentals=1 << 21),
        name="green_tile",
    )(side, places, first)
    part = pl.pallas_call(
        functools.partial(second_kernel, node_count=count),
        out_shape=jax.ShapeDtypeStruct((far, 2, tx, own), bf16),
        in_specs=[VMEM, HBM, VMEM],
        out_specs=VMEM,
        scratch_shapes=[
            pltpu.VMEM((2 * tx, near * own), bf16),
            pltpu.VMEM((near - kept, 2, own, far * own), bf16),
            pltpu.VMEM((2 * tx, far * own), f32),
            pltpu.VMEM((2 * tx, far * own), f32),
            pltpu.SemaphoreType.DMA((3,)),
        ],
        compiler_params=limit(50),
        name="second_wave",
    )(source, tile, tile_near)
    parts = lax.all_to_all(part, REDUCE, split_axis=0, concat_axis=0, tiled=True)
    second, terms = pl.pallas_call(
        functools.partial(last_kernel, share=1.0 / (lanes * tx)),
        out_shape=(
            jax.ShapeDtypeStruct((1, 2, tx, own), bf16),
            jax.ShapeDtypeStruct((lanes, 1, own), f32),
        ),
        in_specs=[VMEM, VMEM],
        out_specs=(VMEM, VMEM),
        compiler_params=limit(4),
        name="last_sum",
    )(parts, first)
    terms = lax.all_to_all(terms, "freq", split_axis=0, concat_axis=0, tiled=True)
    return second, terms.sum(axis=(0, 1))


def solution(mesh):
    split = Mesh(mesh.devices.reshape(2, 2, 8, 4, mesh.shape["freq"]), (*BLK, "freq"))
    in_specs = (P(None, BLK), P(), P(None, BLK), P("freq"))
    out_specs = (P("freq", None, None, BLK), P(BLK))
    return jax.shard_map(local, mesh=split, in_specs=in_specs, out_specs=out_specs, check_vma=False)
```

```python
import functools
import math

import jax
import jax.numpy as jnp
from jax import lax
from jax.experimental import pallas as pl
from jax.experimental.pallas import tpu as pltpu
from jax.sharding import Mesh
from jax.sharding import PartitionSpec as P

GRID = 64
BLK = ("zs", "za", "ys", "ya", "x")
GATHER = ("za", "ya", "x")
REDUCE = ("zs", "ys")
LANES = 128
FEATURES = 16
SOFT = 0.0025 * GRID * GRID


def bf16_parts(x, count):
    parts = []
    for _ in range(count):
        mantissa, exponent = math.frexp(x)
        parts.append(math.ldexp(round(mantissa * 256), exponent - 8))
        x -= parts[-1]
    return parts


SOFT_PARTS = bf16_parts(SOFT, 3)
MAGIC = 12582912.0
KEPT = 4
ROOT2 = math.sqrt(2.0)
SIN_POLY = [ROOT2 * c for c in (3.1415820221197075, -5.167142794757069, 2.541899010399708, -0.554636148527055)]
COS_POLY = [ROOT2 * c for c in (0.9999933001981278, -4.933938170377516, 4.04128504935244, -1.2221298133692595)]


def poly(coefs, s):
    total = coefs[-1] * s + coefs[-2]
    for c in coefs[-3::-1]:
        total = total * s + c
    return total


def green_parts(v, turns_per_step):
    inv = lax.rsqrt(v)
    turns = (v * inv) * turns_per_step
    f = turns - lax.round(turns, lax.RoundingMethod.TO_NEAREST_EVEN)
    s = f * f
    half_sin = poly(SIN_POLY, s) * f
    half_cos = poly(COS_POLY, s)
    q = inv * half_sin
    return inv - q * half_sin, q * half_cos


def split_norm(p):
    n = jnp.sum(p * p, axis=0, keepdims=True)
    high = ((n * (1 / 64) + MAGIC) - MAGIC) * 64.0
    return high, n - high


def features(places, target):
    p = places.astype(jnp.float32) - 32.0
    high, low = split_norm(p)
    one = jnp.ones_like(high)
    zero = jnp.zeros((FEATURES - 7 - len(SOFT_PARTS), p.shape[1]), jnp.float32)
    if target:
        return jnp.concatenate([p, high, low, *[one] * (2 + len(SOFT_PARTS)), zero], axis=0)
    soft = [jnp.full_like(one, c) for c in SOFT_PARTS]
    return jnp.concatenate([p * -2.0, one, one, high, low, *soft, zero], axis=0)


def spread_features(x, y, z):
    lane = lax.broadcasted_iota(jnp.int32, x.shape, 1)
    x, y, z = x - 32.0, y - 32.0, z - 32.0
    n = x * x + y * y + z * z
    high = ((n * (1 / 64) + MAGIC) - MAGIC) * 64.0
    low = n - high
    out = jnp.where(lane == 0, x, 0.0)
    out = jnp.where(lane == 1, y, out)
    out = jnp.where(lane == 2, z, out)
    out = jnp.where(lane == 3, high, out)
    out = jnp.where(lane == 4, low, out)
    return jnp.where((lane >= 5) & (lane < 7 + len(SOFT_PARTS)), 1.0, out)


def dot(a, b, contract=((1,), (0,))):
    return lax.dot_general(a, b, (contract, ((), ())), preferred_element_type=jnp.float32)


def start_kernel(wavenumber_ref, node_ref, emitters_ref, admittance_ref, own_ref, index_ref, side_ref):
    own_ref[...] = features(node_ref[...], True).astype(jnp.bfloat16)
    emitters = jnp.broadcast_to(emitters_ref[...].astype(jnp.float32), (LANES, emitters_ref.shape[1]))
    index_ref[...] = jnp.transpose(emitters).astype(jnp.int32)
    side_ref[0:2] = admittance_ref[...]
    turns = wavenumber_ref[0] * (1.0 / (GRID * 2.0 * math.pi))
    side_ref[2:8] = jnp.full((6, side_ref.shape[1]), turns, jnp.float32)


def first_kernel(side_ref, places_ref, own_ref, index_ref, first_ref, weighted_ref,
                 rows_ref, c0, c1, g0, g1, acc_ref):
    blocks = places_ref.shape[0]
    own = own_ref.shape[1]
    emitters = index_ref.shape[0]
    width = c0.shape[1]
    per = width // own
    chunks = blocks // per
    turns = side_ref[6:7, 0:1]

    rows_ref[0:own, 0:FEATURES] = jnp.transpose(own_ref[...].astype(jnp.float32)).astype(jnp.bfloat16)
    index = index_ref[...]
    lane = lax.broadcasted_iota(jnp.int32, (emitters, LANES), 1)
    of_block = jnp.where(lane == index // own, 1.0, 0.0).astype(jnp.bfloat16)
    at_lane = lane == index % own
    every = jnp.ones((LANES, LANES), jnp.bfloat16)
    found = []
    for d in range(3):
        line = dot(of_block, places_ref[:, d, :])
        found.append(dot(jnp.where(at_lane, line, 0.0).astype(jnp.bfloat16), every))
    rows_ref[own : own + emitters] = spread_features(*found).astype(jnp.bfloat16)

    acc_ref[...] = jnp.zeros_like(acc_ref)

    def columns(chunk, c_ref):
        for b in range(per):
            psi = features(places_ref[chunk * per + b], False)
            c_ref[:, b * own : (b + 1) * own] = psi.astype(jnp.bfloat16)

    def tile(c_ref, g_ref):
        for w in range(0, width, 256):
            psi = c_ref[:, w : w + 256]
            for r in range(0, own + emitters, 64):
                at = r if r < own else r + own
                step = own if r < own else emitters
                real, imag = green_parts(dot(rows_ref[r : r + 64, 0:FEATURES], psi), turns)
                g_ref[at : at + 64, w : w + 256] = real.astype(jnp.bfloat16)
                g_ref[at + step : at + step + 64, w : w + 256] = imag.astype(jnp.bfloat16)

    def gather(g_ref):
        acc_ref[...] += dot(g_ref[2 * own :, :], g_ref[0 : 2 * own, :], ((1,), (1,)))

    columns(0, c0)
    g1[...] = jnp.zeros_like(g1)

    def pair(i, carry):
        columns(2 * i + 1, c1)
        tile(c0, g0)
        gather(g1)
        columns(jnp.minimum(2 * i + 2, chunks - 1), c0)
        tile(c1, g1)
        gather(g0)
        return carry

    lax.fori_loop(0, chunks // 2, pair, 0)
    gather(g1)
    scale = (GRID * GRID) * float(blocks * own) ** (-0.5)
    top, low = acc_ref[0:emitters, :], acc_ref[emitters:, :]
    real = (top[:, 0:own] - low[:, own:]) * scale
    imag = (low[:, 0:own] + top[:, own:]) * scale
    first_ref[0] = real
    first_ref[1] = imag
    a, b = side_ref[0:1, :], side_ref[1:2, :]
    w_real = (a * real - b * imag).astype(jnp.bfloat16)
    w_imag = (a * imag + b * real).astype(jnp.bfloat16)
    for k in range(weighted_ref.shape[0]):
        weighted_ref[k, 0] = w_real
        weighted_ref[k, 1] = w_imag


def block_at(where, sizes):
    place = 0
    for a in BLK:
        place = place * sizes[a] + where[a]
    return place


def unravel(k, axes, sizes):
    where = {}
    for a in reversed(axes):
        where[a] = k % sizes[a]
        k = k // sizes[a]
    return where


def tile_kernel(side_ref, places_ref, after_ref, tile_ref, near_ref, cols_ref, d0, d1, t0, t1, sems, *, sizes):
    here = {a: lax.axis_index(a) for a in BLK}
    own = places_ref.shape[2]
    far = tile_ref.shape[0]
    groups = far + near_ref.shape[0]
    width = tile_ref.shape[3]
    turns = side_ref[6:7, 0:1]
    for b in range(width // own):
        block = block_at({**here, **unravel(b, REDUCE, sizes)}, sizes)
        cols_ref[:, b * own : (b + 1) * own] = features(places_ref[block], True).astype(jnp.bfloat16)

    def distances(c, d_ref):
        block = block_at({**here, **unravel(c, GATHER, sizes)}, sizes)
        d_ref[:, 0:FEATURES] = jnp.transpose(features(places_ref[block], False)).astype(jnp.bfloat16)

    def tile(d_ref, store):
        for w in range(0, width, 256):
            targets = cols_ref[:, w : w + 256]
            for r in range(0, own, 64):
                real, imag = green_parts(dot(d_ref[r : r + 64, 0:FEATURES], targets), turns)
                store(0, r, w, real.astype(jnp.bfloat16))
                store(1, r, w, imag.astype(jnp.bfloat16))

    def into(t_ref):
        def store(p, r, w, value):
            t_ref[p, r : r + 64, w : w + 256] = value

        return store

    def kept(c):
        def store(p, r, w, value):
            near_ref[c, p, r : r + 64, w : w + 256] = value

        return store

    def out(c, t_ref, s):
        half = own // 2
        return [
            pltpu.make_async_copy(
                t_ref.at[p, h * half : (h + 1) * half], tile_ref.at[c, p, h * half : (h + 1) * half], sems.at[s, p, h]
            )
            for p in range(2)
            for h in range(2)
        ]

    distances(0, d0)

    def pair(k, carry):
        @pl.when(k > 0)
        def _():
            for copy in out(2 * k - 2, t0, 0):
                copy.wait()

        distances(2 * k + 1, d1)
        tile(d0, into(t0))
        for copy in out(2 * k, t0, 0):
            copy.start()

        @pl.when(k > 0)
        def _():
            for copy in out(2 * k - 1, t1, 1):
                copy.wait()

        distances(jnp.minimum(2 * k + 2, groups - 1), d0)
        tile(d1, into(t1))
        for copy in out(2 * k + 1, t1, 1):
            copy.start()
        return carry

    lax.fori_loop(0, far // 2, pair, 0)

    def last(k, carry):
        distances(far + 2 * k + 1, d1)
        tile(d0, kept(2 * k))
        distances(jnp.minimum(far + 2 * k + 2, groups - 1), d0)
        tile(d1, kept(2 * k + 1))
        return carry

    lax.fori_loop(0, (groups - far) // 2, last, 0)
    for copy in out(far - 2, t0, 0) + out(far - 1, t1, 1):
        copy.wait()


def second_kernel(source_ref, tile_ref, near_ref, part_ref, lhs_ref, all_ref, acc_r, acc_i, sems, *, node_count):
    groups, _, emitters, own = source_ref.shape
    targets = part_ref.shape[0]
    far = tile_ref.shape[0]
    per = far // sems.shape[0]

    def bring(p):
        at = pl.ds(p * per, per)
        return pltpu.make_async_copy(tile_ref.at[at], all_ref.at[at], sems.at[p])

    for p in range(far // per):
        bring(p).start()
    for c in range(groups):
        lhs_ref[:, c * own : (c + 1) * own] = source_ref[c].reshape(2 * emitters, own)
    for begin, count in [(far, groups - far), *((p, per) for p in range(0, far, per))]:
        if begin < far:
            bring(begin // per).wait()
        lhs = lhs_ref[:, begin * own : (begin + count) * own]
        for part, acc in ((0, acc_r), (1, acc_i)):
            held = near_ref[:, part] if begin == far else all_ref[begin : begin + count, part]
            here = dot(lhs, held.reshape(count * own, targets * own))
            acc[...] = here if begin == far else acc[...] + here
    scale = GRID * float(node_count) ** (-0.5)
    for b in range(targets):
        at = slice(b * own, (b + 1) * own)
        part_ref[b, 0] = ((acc_r[0:emitters, at] - acc_i[emitters:, at]) * scale).astype(part_ref.dtype)
        part_ref[b, 1] = ((acc_r[emitters:, at] + acc_i[0:emitters, at]) * scale).astype(part_ref.dtype)


def last_kernel(parts_ref, first_ref, second_ref, terms_ref, *, share):
    real = parts_ref[0, 0].astype(jnp.float32)
    imag = parts_ref[0, 1].astype(jnp.float32)
    for b in range(1, parts_ref.shape[0]):
        real += parts_ref[b, 0].astype(jnp.float32)
        imag += parts_ref[b, 1].astype(jnp.float32)
    second_ref[0, 0] = real.astype(jnp.bfloat16)
    second_ref[0, 1] = imag.astype(jnp.bfloat16)
    terms = jnp.sum(first_ref[0] * real - first_ref[1] * imag, axis=0, keepdims=True) * share
    terms_ref[...] = jnp.broadcast_to(terms[None], terms_ref.shape)


VMEM = pl.BlockSpec(memory_space=pltpu.VMEM)
HBM = pl.BlockSpec(memory_space=pltpu.HBM)
SMEM = pl.BlockSpec(memory_space=pltpu.SMEM)


def limit(mib):
    return pltpu.CompilerParams(vmem_limit_bytes=mib << 20)


def local(node_index, emitters, admittance, wavenumbers):
    sizes = {a: lax.axis_size(a) for a in BLK}
    blocks = math.prod(sizes.values())
    lanes = lax.axis_size("freq")
    own = node_index.shape[1]
    count = blocks * own
    tx = emitters.shape[0]
    near, far = lax.axis_size(GATHER), lax.axis_size(REDUCE)

    f32, bf16 = jnp.float32, jnp.bfloat16
    copies = jnp.broadcast_to(node_index.astype(bf16), (blocks, *node_index.shape))
    places = lax.all_to_all(copies, BLK, split_axis=0, concat_axis=0, tiled=True)
    own_features, index, side = pl.pallas_call(
        start_kernel,
        out_shape=(
            jax.ShapeDtypeStruct((FEATURES, own), bf16),
            jax.ShapeDtypeStruct((tx, LANES), jnp.int32),
            jax.ShapeDtypeStruct((8, own), f32),
        ),
        in_specs=[SMEM, VMEM, VMEM, VMEM],
        out_specs=(VMEM,) * 3,
        compiler_params=limit(4),
        name="start",
    )(wavenumbers, node_index, emitters[None], admittance)
    width = 16 * own
    first, weighted = pl.pallas_call(
        first_kernel,
        out_shape=(
            jax.ShapeDtypeStruct((2, tx, own), f32),
            jax.ShapeDtypeStruct((near, 2, tx, own), bf16),
        ),
        in_specs=[VMEM] * 4,
        out_specs=(VMEM, VMEM),
        scratch_shapes=[
            pltpu.VMEM((own + tx, LANES), bf16),
            pltpu.VMEM((FEATURES, width), bf16),
            pltpu.VMEM((FEATURES, width), bf16),
            pltpu.VMEM((2 * (own + tx), width), bf16),
            pltpu.VMEM((2 * (own + tx), width), bf16),
            pltpu.VMEM((2 * tx, 2 * own), f32),
        ],
        compiler_params=limit(12),
        name="first_wave",
    )(side, places, own_features, index)

    source = lax.all_to_all(weighted, GATHER, split_axis=0, concat_axis=0, tiled=True)
    kept = KEPT
    tile, tile_near = pl.pallas_call(
        functools.partial(tile_kernel, sizes=sizes),
        out_shape=(
            jax.ShapeDtypeStruct((near - kept, 2, own, far * own), bf16),
            jax.ShapeDtypeStruct((kept, 2, own, far * own), bf16),
        ),
        in_specs=[VMEM, VMEM, pl.BlockSpec(memory_space=pl.ANY)],
        out_specs=(HBM, VMEM),
        scratch_shapes=[
            pltpu.VMEM((FEATURES, far * own), bf16),
            pltpu.VMEM((own, LANES), bf16),
            pltpu.VMEM((own, LANES), bf16),
            pltpu.VMEM((2, own, far * own), bf16),
            pltpu.VMEM((2, own, far * own), bf16),
            pltpu.SemaphoreType.DMA((2, 2, 2)),
        ],
        compiler_params=limit(50),
        cost_estimate=pl.CostEstimate(flops=10**10, bytes_accessed=1 << 23, transcendentals=1 << 21),
        name="green_tile",
    )(side, places, first)
    part = pl.pallas_call(
        functools.partial(second_kernel, node_count=count),
        out_shape=jax.ShapeDtypeStruct((far, 2, tx, own), bf16),
        in_specs=[VMEM, HBM, VMEM],
        out_specs=VMEM,
        scratch_shapes=[
            pltpu.VMEM((2 * tx, near * own), bf16),
            pltpu.VMEM((near - kept, 2, own, far * own), bf16),
            pltpu.VMEM((2 * tx, far * own), f32),
            pltpu.VMEM((2 * tx, far * own), f32),
            pltpu.SemaphoreType.DMA((6,)),
        ],
        compiler_params=limit(50),
        name="second_wave",
    )(source, tile, tile_near)
    parts = lax.all_to_all(part, REDUCE, split_axis=0, concat_axis=0, tiled=True)
    second, terms = pl.pallas_call(
        functools.partial(last_kernel, share=1.0 / (lanes * tx)),
        out_shape=(
            jax.ShapeDtypeStruct((1, 2, tx, own), bf16),
            jax.ShapeDtypeStruct((lanes, 1, own), f32),
        ),
        in_specs=[VMEM, VMEM],
        out_specs=(VMEM, VMEM),
        compiler_params=limit(4),
        name="last_sum",
    )(parts, first)
    terms = lax.all_to_all(terms, "freq", split_axis=0, concat_axis=0, tiled=True)
    return second, terms.sum(axis=(0, 1))


def solution(mesh):
    split = Mesh(mesh.devices.reshape(2, 2, 4, 2, 4, mesh.shape["freq"]), (*BLK, "freq"))
    in_specs = (P(None, BLK), P(), P(None, BLK), P("freq"))
    out_specs = (P("freq", None, None, BLK), P(BLK))
    return jax.shard_map(local, mesh=split, in_specs=in_specs, out_specs=out_specs, check_vma=False)
```
